32 devices in a mesh: gx: 4 (over y, x), gy: 8 (over z, core).
Axes of the slice: x: 2, y: 2, z: 4, core: 2. Of those that a mesh axis runs over, the one named last changes fastest.
Arguments:
- density: float32 [16, 256, 1024], P(None, 'gx', 'gy'), may hold values from 0.1 to 1
- cotangent: float32 [16, 256, 1024], P(None, 'gx', 'gy'), may hold values from -6 to 6
Outputs:
- printed: float32 [16, 256, 1024], P(None, 'gx', 'gy')
- gradient: float32 [16, 256, 1024], P(None, 'gx', 'gy')
The draws below stay inside these ranges and needn't reach their ends.
All inputs are finite; a program needn't handle non-finite values.
Results may differ from the reference program's by a relative error of at most 0.0003.
Values sent between devices are 32-bit elements; how exact they have to be, the bound alone decides.
No kernel may reach another device: no remote copies, remote signals or barrier semaphores. Data moves between devices by JAX's collectives and lax.ppermute only.
A program may use at most 64 MiB of HBM per device.

```python
import math
import jax
import jax.numpy as jnp
from jax import lax

NZ = 16
NX = 256
NY = 1024


def draw_density(key, part):
    key_pillar = jax.random.fold_in(key, 11)
    key_level = jax.random.fold_in(key, 23)
    picks = jax.random.randint(key_pillar, (NX, NY), 0, 400)
    pillar = picks == 0
    spread = jax.random.uniform(key_level, (NZ, NX, NY), jnp.float32)
    upper = 0.85 + 0.15 * spread
    base = 0.1 + 0.1 * spread
    summit = 0.95 + 0.05 * spread
    ground = jnp.where(pillar[None], summit, base)
    layers = jnp.arange(NZ, dtype=jnp.int32)[:, None, None]
    return jnp.where(layers == 0, ground, upper).astype(jnp.float32)


def steps_of(key, shape, cuts, low, high):
    gain = 1.0
    for position, blocks in cuts:
        draws = jax.random.uniform(jax.random.fold_in(jax.random.fold_in(key, 6), position), (blocks,), jnp.float32, low / len(cuts), high / len(cuts))
        gain = gain * jnp.repeat(jnp.exp(draws), shape[position] // blocks).reshape((-1,) + (1,) * (len(shape) - 1 - position))
    return gain


def centred(own_key, dims, deviation, most, pieces=(), held_as=jnp.bfloat16):
    entries = jax.random.normal(own_key, dims, jnp.float32) * deviation
    if len(pieces) > 0:
        entries = steps_of(own_key, dims, pieces, -0.22, 0.18) * entries
    return jnp.clip(entries, min=-most, max=most).astype(held_as)


def setup_inputs(seed: int = 0) -> dict:
    seeds = jax.random.split(jax.random.key(seed), 3)
    density = draw_density(jax.random.fold_in(seeds[2], 71), 0)
    cotangent = centred(seeds[1], (NZ, NX, NY), 1.0, 6.0, ((1, 4), (2, 8)), jnp.float32)
    return dict(density=density, cotangent=cotangent)


power_p = 20.0
root_q = 20.0 + math.log(5.0) / math.log(0.1)
smooth_eps = 0.0001

def cross_roll(plane):
    return plane + jnp.roll(plane, 1, 0) + jnp.roll(plane, -1, 0) + jnp.roll(plane, 1, 1) + jnp.roll(plane, -1, 1)

def reference(density, cotangent):
    layers = jnp.arange(density.shape[0], dtype=jnp.int32)

    def forward(prev, inputs):
        plane, zval = inputs
        total = cross_roll(prev ** power_p)
        level = jnp.where(zval == 0, jnp.float32(1.0), total ** (1.0 / root_q))
        diff = plane - level
        printed_layer = 0.5 * (plane + level - jnp.sqrt(diff * diff + smooth_eps) + math.sqrt(smooth_eps))
        return (printed_layer, printed_layer)
    start = jnp.ones(density.shape[1:], jnp.float32)
    last, printed = lax.scan(forward, start, (density, layers))
    below = jnp.concatenate([start[None], printed[:-1]], 0)

    def backward(carried, inputs):
        grad_in, plane, here, under, zval = inputs
        adjoint = grad_in + power_p / root_q * here ** (power_p - 1.0) * cross_roll(carried)
        total = cross_roll(under ** power_p)
        level = jnp.where(zval == 0, jnp.float32(1.0), total ** (1.0 / root_q))
        diff = plane - level
        root = jnp.sqrt(diff * diff + smooth_eps)
        grad_layer = adjoint * 0.5 * (1.0 - diff / root)
        carried_next = adjoint * 0.5 * (1.0 + diff / root) * level / total
        return (carried_next, grad_layer)
    zero_state = jnp.zeros(density.shape[1:], jnp.float32)
    final, gradient = lax.scan(backward, zero_state, (cotangent, density, printed, below, layers), reverse=True)
    return (printed, gradient)
```

```python
import functools
import math

import jax
import jax.numpy as jnp
from jax import lax
from jax.experimental import pallas as pl
from jax.experimental.pallas import tpu as pltpu
from jax.sharding import PartitionSpec as P

power_p = 20.0
root_q = 20.0 + math.log(5.0) / math.log(0.1)
smooth_eps = 0.0001
SUB = 8

VMEM = pl.BlockSpec(memory_space=pltpu.VMEM)


def up8(n):
    return -(-n // SUB) * SUB


class Plan:
    def __init__(self, layers, rows, cols):
        self.nz, self.rows, self.cols = layers, rows, cols
        self.fields = [(0, z, 2 * (layers - 1) - z) for z in range(layers)]
        self.fields += [(1, z, z) for z in range(layers - 1, 0, -1)]
        far = 2 * (layers - 1)
        self.halo = up8(far)
        self.row_at = {}
        at = SUB
        for arr, z, d in self.fields:
            self.row_at[arr, z] = at
            at += d
        self.row_len = up8(at) + SUB
        self.col_at, self.col_tiles = self.fit([((arr, z), d) for arr, z, d in self.fields])
        items = []
        for arr, z, d in self.fields:
            for k in range(-(-(d - 1) // SUB)):
                items.append(((arr, z, k), 2 * (d - 1 - SUB * k)))
        self.corner_at, self.corner_tiles = self.fit(items)

    def fit(self, items):
        room, where = [], {}
        for key, width in sorted(items, key=lambda item: -item[1]):
            for tile, used in enumerate(room):
                if used + width <= self.cols:
                    break
            else:
                tile = len(room)
                room.append(0)
            where[key] = (tile, room[tile])
            room[tile] += width
        return where, len(room)


def shift(x, amount):
    amount %= x.shape[1]
    return x if amount == 0 else pltpu.roll(x, amount, 1)


def lanes_of(shape):
    return lax.broadcasted_iota(jnp.int32, shape, 1)


def pack_rows(plan, dens, cot, first, last):
    for arr, z, d in plan.fields:
        src = (dens, cot)[arr]
        at = plan.row_at[arr, z]
        first[at : at + d, :] = src[z, :d, :]
        last[at : at + d, :] = src[z, plan.rows - d :, :]
    end = plan.row_at[1, 1] + 1
    for ref in (first, last):
        ref[:SUB, :] = jnp.zeros((SUB, plan.cols), jnp.float32)
        ref[end:, :] = jnp.zeros((plan.row_len - end, plan.cols), jnp.float32)


def pack_columns(plan, dens, cot, first, last):
    n = plan.cols
    lane = lanes_of((SUB, n))
    for tile in range(plan.col_tiles):
        inside = [f for f in plan.fields if plan.col_at[f[0], f[1]][0] == tile]
        inside.sort(key=lambda f: plan.col_at[f[0], f[1]][1])
        for r in range(0, plan.rows, SUB):
            one, two = None, None
            for arr, z, d in inside:
                at = plan.col_at[arr, z][1]
                x = (dens, cot)[arr][z, r : r + SUB, :]
                a, b = shift(x, at), shift(x, at + d)
                if one is None:
                    one, two = a, b
                else:
                    here = lane >= at
                    one, two = jnp.where(here, a, one), jnp.where(here, b, two)
            first[tile, r : r + SUB, :] = one
            last[tile, r : r + SUB, :] = two


def pack_corners(plan, left, right, first, last):
    lane = lanes_of((SUB, plan.cols))
    out = [[None] * plan.corner_tiles, [None] * plan.corner_tiles]
    order = sorted(plan.corner_at.items(), key=lambda item: item[1][1])
    reach = {(arr, z): d for arr, z, d in plan.fields}
    for (arr, z, k), (tile, at) in order:
        d = reach[arr, z]
        w = d - 1 - SUB * k
        ctile, cat = plan.col_at[arr, z]
        for way in range(2):
            r = SUB * k if way == 0 else plan.rows - SUB * (k + 1)
            a = shift(left[ctile, r : r + SUB, :], at - (cat + d - w))
            b = shift(right[ctile, r : r + SUB, :], at + w - cat)
            both = jnp.where(lane >= at + w, b, a)
            prev = out[way][tile]
            out[way][tile] = both if prev is None else jnp.where(lane >= at, both, prev)
    for tile in range(plan.corner_tiles):
        first[tile] = out[0][tile]
        last[tile] = out[1][tile]


def assemble(plan, arr, src, above, below, left, right, cabove, cbelow, main, side):
    n, top = plan.cols, plan.halo
    lane = lanes_of((SUB, n))
    low = lane < n // 2
    for a, z, d in plan.fields:
        if a != arr:
            continue
        at = plan.row_at[arr, z]
        ctile, cat = plan.col_at[arr, z]
        for r in range(0, plan.rows, SUB):
            main[z, top + r : top + r + SUB, :] = src[z, r : r + SUB, :]
            x = shift(left[ctile, r : r + SUB, :], -(cat + d))
            y = shift(right[ctile, r : r + SUB, :], -cat)
            side[z, top + r : top + r + SUB, :] = jnp.where(low, y, x)
        for k in range(-(-d // SUB)):
            lo, hi = top - SUB * (k + 1), top + plan.rows + SUB * k
            main[z, lo : lo + SUB, :] = above[at + d - SUB * (k + 1) : at + d - SUB * k, :]
            main[z, hi : hi + SUB, :] = below[at + SUB * k : at + SUB * (k + 1), :]
            w = d - 1 - SUB * k
            if w > 0:
                tile, cor = plan.corner_at[arr, z, k]
                side[z, lo : lo + SUB, :] = shift(cabove[tile], -(cor + w))
                side[z, hi : hi + SUB, :] = shift(cbelow[tile], -(cor + w))


def cross(ref, now, r, lane):
    n = lane.shape[1]
    b = SUB + r
    m, s = ref[now, 0, b : b + SUB, :], ref[now, 1, b : b + SUB, :]
    vm = ref[now, 0, b - 1 : b + SUB - 1, :] + ref[now, 0, b + 1 : b + SUB + 1, :]
    vs = ref[now, 1, b - 1 : b + SUB - 1, :] + ref[now, 1, b + 1 : b + SUB + 1, :]
    m1, s1 = pltpu.roll(m, 1, 1), pltpu.roll(s, 1, 1)
    m2, s2 = pltpu.roll(m, n - 1, 1), pltpu.roll(s, n - 1, 1)
    start, end = lane == 0, lane == n - 1
    hm = jnp.where(start, s1, m1) + jnp.where(end, s2, m2)
    hs = jnp.where(start, m1, s1) + jnp.where(end, m2, s2)
    return m + vm + hm, s + vs + hs


def filter_body(
    plan, dens, cot, above, below, left, right, cabove, cbelow,
    printed, gradient, dm, ds, cm, cs, work, slope, weight, da,
):
    nz, rows, n, top = plan.nz, plan.rows, plan.cols, plan.halo
    lane = lanes_of((SUB, n))
    full = top + rows + top
    args = (above, below, left, right, cabove, cbelow)
    assemble(plan, 0, dens, *args, dm, ds)
    assemble(plan, 1, cot, *args, cm, cs)

    margin = jnp.ones((SUB, n), jnp.float32)
    for now in range(2):
        for half in range(2):
            work[now, half, :SUB, :] = margin
            work[now, half, SUB + full :, :] = margin

    def tiles(reach):
        depth = up8(max(reach, 0))
        return range(top - depth, top + rows + depth, SUB)

    coef_rows = up8(nz - 1)

    def layer(z, now, r, half, density, total):
        if total is None:
            level = jnp.ones_like(density)
        else:
            lg = jnp.log(total)
            level = jnp.exp2(lg * jnp.float32(1.0 / (root_q * math.log(2.0))))
            ratio = jnp.exp2(lg * jnp.float32((1.0 / root_q - 1.0) / math.log(2.0)))
        diff = density - level
        square = diff * diff + smooth_eps
        inv = lax.rsqrt(square)
        u = diff * inv
        out = 0.5 * (density + level - square * inv + math.sqrt(smooth_eps))
        p2 = out * out
        p4 = p2 * p2
        p16 = (p4 * p4) * (p4 * p4)
        work[now, half, SUB + r : SUB + r + SUB, :] = p16 * p4
        if top - coef_rows <= r < top + rows + coef_rows:
            slope[z, half, r : r + SUB, :] = jnp.float32(power_p / root_q) * (p16 * (p2 * out))
            if total is not None:
                weight[z, half, r : r + SUB, :] = (0.5 + 0.5 * u) * ratio
        if half == 0 and top <= r < top + rows:
            printed[z, r - top : r - top + SUB, :] = out
            da[z, r - top : r - top + SUB, :] = 0.5 - 0.5 * u

    for r in tiles(2 * (nz - 1)):
        layer(0, 0, r, 0, dm[0, r : r + SUB, :], None)
        layer(0, 0, r, 1, ds[0, r : r + SUB, :], None)

    def forward(reach):
        def step(z, carry):
            now = lax.rem(z, 2)
            for r in tiles(reach):
                tm, ts = cross(work, 1 - now, r, lane)
                layer(z, now, r, 0, dm[z, r : r + SUB, :], tm)
                layer(z, now, r, 1, ds[z, r : r + SUB, :], ts)
            return carry

        return step

    def ranges(reach_of, zs):
        runs = []
        for z in zs:
            if runs and up8(reach_of(z)) == up8(reach_of(runs[-1][0])):
                runs[-1][1] = z
            else:
                runs.append([z, z])
        return runs

    for lo, hi in ranges(lambda z: 2 * (nz - 1) - z, range(1, nz)):
        lax.fori_loop(lo, hi + 1, forward(2 * (nz - 1) - lo), 0)

    def back(z, now, r, total):
        inside = top <= r < top + rows
        for half, spread in enumerate(total):
            adjoint = (cm, cs)[half][z, r : r + SUB, :]
            if spread is not None:
                adjoint = adjoint + slope[z, half, r : r + SUB, :] * spread
            work[now, half, SUB + r : SUB + r + SUB, :] = adjoint * weight[z, half, r : r + SUB, :]
            if half == 0 and inside:
                k = r - top
                gradient[z, k : k + SUB, :] = adjoint * da[z, k : k + SUB, :]

    for r in tiles(nz - 1):
        back(nz - 1, (nz - 1) % 2, r, (None, None))

    def backward(reach):
        def step(i, carry):
            z = nz - 1 - i
            now = lax.rem(z, 2)
            for r in tiles(reach):
                back(z, now, r, cross(work, 1 - now, r, lane))
            return carry

        return step

    for lo, hi in ranges(lambda z: z, range(nz - 2, 0, -1)):
        lax.fori_loop(nz - 1 - lo, nz - hi, backward(lo), 0)

    for r in range(top, top + rows, SUB):
        spread, _ = cross(work, 1, r, lane)
        k = r - top
        adjoint = cot[0, k : k + SUB, :] + slope[0, 0, r : r + SUB, :] * spread
        gradient[0, k : k + SUB, :] = adjoint * da[0, k : k + SUB, :]


def call(body, outs, n_in, scratch=(), flops=1000):
    return pl.pallas_call(
        body,
        out_shape=[jax.ShapeDtypeStruct(s, jnp.float32) for s in outs],
        in_specs=[VMEM] * n_in,
        out_specs=[VMEM] * len(outs),
        scratch_shapes=[pltpu.VMEM(s, jnp.float32) for s in scratch],
        cost_estimate=pl.CostEstimate(flops=flops, bytes_accessed=flops, transcendentals=0),
    )


def swap(axis, first, last):
    count = lax.axis_size(axis)
    forward = [(i, (i + 1) % count) for i in range(count)]
    backward = [(i, (i - 1) % count) for i in range(count)]
    return lax.ppermute(last, axis, forward), lax.ppermute(first, axis, backward)


def shards(density, cotangent):
    nz, rows, cols = density.shape
    plan = Plan(nz, rows, cols)
    part = functools.partial
    first, last = call(part(pack_rows, plan), [(plan.row_len, cols)] * 2, 2)(density, cotangent)
    above, below = swap("gx", first, last)
    first, last = call(part(pack_columns, plan), [(plan.col_tiles, rows, cols)] * 2, 2)(density, cotangent)
    left, right = swap("gy", first, last)
    first, last = call(part(pack_corners, plan), [(plan.corner_tiles, SUB, cols)] * 2, 2)(left, right)
    cabove, cbelow = swap("gx", first, last)
    full = rows + 2 * plan.halo
    scratch = [(nz, full, cols)] * 4
    scratch += [(2, 2, full + 2 * SUB, cols), (nz, 2, full, cols), (nz, 2, full, cols), (nz, rows, cols)]
    body = call(part(filter_body, plan), [(nz, rows, cols)] * 2, 8, scratch)
    return tuple(body(density, cotangent, above, below, left, right, cabove, cbelow))


def solution(mesh):
    placed = P(None, "gx", "gy")
    return jax.shard_map(
        shards,
        mesh=mesh,
        in_specs=(placed, placed),
        out_specs=(placed, placed),
        check_vma=False,
    )
```

```python
import functools
import math

import jax
import jax.numpy as jnp
from jax import lax
from jax.experimental import pallas as pl
from jax.experimental.pallas import tpu as pltpu
from jax.sharding import PartitionSpec as P

power_p = 20.0
root_q = 20.0 + math.log(5.0) / math.log(0.1)
smooth_eps = 0.0001
SUB = 8

VMEM = pl.BlockSpec(memory_space=pltpu.VMEM)


def up8(n):
    return -(-n // SUB) * SUB


class Plan:
    def __init__(self, layers, rows, cols):
        self.nz, self.rows, self.cols = layers, rows, cols
        self.fields = [(0, z, 2 * (layers - 1) - z) for z in range(layers)]
        self.fields += [(1, z, z) for z in range(layers - 1, 0, -1)]
        far = 2 * (layers - 1)
        self.halo = up8(far)
        self.row_at = {}
        at = SUB
        for arr, z, d in self.fields:
            self.row_at[arr, z] = at
            at += d
        self.row_len = up8(at) + SUB
        self.col_at, self.col_tiles = self.fit([((arr, z), d) for arr, z, d in self.fields])
        items = []
        for arr, z, d in self.fields:
            for k in range(-(-(d - 1) // SUB)):
                items.append(((arr, z, k), 2 * (d - 1 - SUB * k)))
        self.corner_at, self.corner_tiles = self.fit(items)

    def fit(self, items):
        room, where = [], {}
        for key, width in sorted(items, key=lambda item: -item[1]):
            for tile, used in enumerate(room):
                if used + width <= self.cols:
                    break
            else:
                tile = len(room)
                room.append(0)
            where[key] = (tile, room[tile])
            room[tile] += width
        return where, len(room)


def shift(x, amount):
    amount %= x.shape[1]
    return x if amount == 0 else pltpu.roll(x, amount, 1)


def lanes_of(shape):
    return lax.broadcasted_iota(jnp.int32, shape, 1)


def pack_rows(plan, dens, cot, first, last):
    for arr, z, d in plan.fields:
        src = (dens, cot)[arr]
        at = plan.row_at[arr, z]
        first[at : at + d, :] = src[z, :d, :]
        last[at : at + d, :] = src[z, plan.rows - d :, :]
    end = plan.row_at[1, 1] + 1
    for ref in (first, last):
        ref[:SUB, :] = jnp.zeros((SUB, plan.cols), jnp.float32)
        ref[end:, :] = jnp.zeros((plan.row_len - end, plan.cols), jnp.float32)


def pack_columns(plan, dens, cot, first, last):
    n = plan.cols
    lane = lanes_of((SUB, n))
    for tile in range(plan.col_tiles):
        inside = [f for f in plan.fields if plan.col_at[f[0], f[1]][0] == tile]
        inside.sort(key=lambda f: plan.col_at[f[0], f[1]][1])
        for r in range(0, plan.rows, SUB):
            one, two = None, None
            for arr, z, d in inside:
                at = plan.col_at[arr, z][1]
                x = (dens, cot)[arr][z, r : r + SUB, :]
                a, b = shift(x, at), shift(x, at + d)
                if one is None:
                    one, two = a, b
                else:
                    here = lane >= at
                    one, two = jnp.where(here, a, one), jnp.where(here, b, two)
            first[tile, r : r + SUB, :] = one
            last[tile, r : r + SUB, :] = two


def pack_corners(plan, left, right, first, last):
    lane = lanes_of((SUB, plan.cols))
    out = [[None] * plan.corner_tiles, [None] * plan.corner_tiles]
    order = sorted(plan.corner_at.items(), key=lambda item: item[1][1])
    reach = {(arr, z): d for arr, z, d in plan.fields}
    for (arr, z, k), (tile, at) in order:
        d = reach[arr, z]
        w = d - 1 - SUB * k
        ctile, cat = plan.col_at[arr, z]
        for way in range(2):
            r = SUB * k if way == 0 else plan.rows - SUB * (k + 1)
            a = shift(left[ctile, r : r + SUB, :], at - (cat + d - w))
            b = shift(right[ctile, r : r + SUB, :], at + w - cat)
            both = jnp.where(lane >= at + w, b, a)
            prev = out[way][tile]
            out[way][tile] = both if prev is None else jnp.where(lane >= at, both, prev)
    for tile in range(plan.corner_tiles):
        first[tile] = out[0][tile]
        last[tile] = out[1][tile]


def unpack_columns(plan, left, right, *sides):
    n = plan.cols
    low = lanes_of((SUB, n)) < n // 2
    for arr, z, d in plan.fields:
        tile, at = plan.col_at[arr, z]
        for r in range(0, plan.rows, SUB):
            x = shift(left[tile, r : r + SUB, :], -(at + d))
            y = shift(right[tile, r : r + SUB, :], -at)
            sides[arr][z, r : r + SUB, :] = jnp.where(low, y, x)


def unpack_halo(plan, arr, above, below, cabove, cbelow, main, side):
    top = plan.halo
    for a, z, d in plan.fields:
        if a != arr:
            continue
        at = plan.row_at[arr, z]
        for k in range(-(-d // SUB)):
            lo, hi = top - SUB * (k + 1), top + SUB * k
            main[z, lo : lo + SUB, :] = above[at + d - SUB * (k + 1) : at + d - SUB * k, :]
            main[z, hi : hi + SUB, :] = below[at + SUB * k : at + SUB * (k + 1), :]
            w = d - 1 - SUB * k
            if w > 0:
                tile, cor = plan.corner_at[arr, z, k]
                side[z, lo : lo + SUB, :] = shift(cabove[tile], -(cor + w))
                side[z, hi : hi + SUB, :] = shift(cbelow[tile], -(cor + w))


def cross(ref, r, lane):
    n = lane.shape[1]
    b = SUB + r
    m, s = ref[0, b : b + SUB, :], ref[1, b : b + SUB, :]
    m1, s1 = pltpu.roll(m, 1, 1), pltpu.roll(s, 1, 1)
    m2, s2 = pltpu.roll(m, n - 1, 1), pltpu.roll(s, n - 1, 1)
    vm = m + ref[0, b - 1 : b + SUB - 1, :] + ref[0, b + 1 : b + SUB + 1, :]
    vs = s + ref[1, b - 1 : b + SUB - 1, :] + ref[1, b + 1 : b + SUB + 1, :]
    start, end = lane == 0, lane == n - 1
    hm = jnp.where(start, s1, m1) + jnp.where(end, s2, m2)
    hs = jnp.where(start, m1, s1) + jnp.where(end, m2, s2)
    return vm + hm, vs + hs


def filter_body(
    plan, dens, cot, dens_side, cot_side, above, below, cabove, cbelow,
    printed_out, gradient_out, dmh, dsh, cmh, csh, even, odd, slope, weight, da, printed, gradient, sems,
):
    nz, rows, n, top = plan.nz, plan.rows, plan.cols, plan.halo
    lane = lanes_of((SUB, n))
    full = top + rows + top
    unpack_halo(plan, 0, above, below, cabove, cbelow, dmh, dsh)

    margin = jnp.ones((SUB, n), jnp.float32)
    for ref in (even, odd):
        for half in range(2):
            ref[half, :SUB, :] = margin
            ref[half, SUB + full :, :] = margin

    def tiles(reach):
        depth = up8(max(reach, 0))
        return range(top - depth, top + rows + depth, SUB)

    def inside(r):
        return top <= r < top + rows

    def field(blocks, halos, half, z, r):
        if inside(r):
            return blocks[half][z, r - top : r - top + SUB, :]
        at = r if r < top else r - rows
        return halos[half][z, at : at + SUB, :]

    coef = up8(nz - 1)

    def layer(z, out, r, half, total):
        density = field((dens, dens_side), (dmh, dsh), half, z, r)
        if total is None:
            level = jnp.ones_like(density)
        else:
            lg = jnp.log(total)
            level = jnp.exp2(lg * jnp.float32(1.0 / (root_q * math.log(2.0))))
        diff = density - level
        square = diff * diff + smooth_eps
        inv = lax.rsqrt(square)
        value = 0.5 * (density + level - square * inv + math.sqrt(smooth_eps))
        p2 = value * value
        p4 = p2 * p2
        p16 = (p4 * p4) * (p4 * p4)
        out[half, SUB + r : SUB + r + SUB, :] = p16 * p4
        if top - coef <= r < top + rows + coef:
            hu = 0.5 * (diff * inv)
            slope[z, half, r : r + SUB, :] = jnp.float32(power_p / root_q) * (p16 * (p2 * value))
            if total is not None:
                ratio = jnp.exp2(lg * jnp.float32((1.0 / root_q - 1.0) / math.log(2.0)))
                weight[z, half, r : r + SUB, :] = (0.5 + hu) * ratio
            if half == 0 and inside(r):
                printed[z, r - top : r - top + SUB, :] = value
                da[z, r - top : r - top + SUB, :] = 0.5 - hu

    for r in tiles(2 * (nz - 1)):
        for half in range(2):
            layer(0, even, r, half, None)

    refs = (even, odd)

    def forward(z, parity, reach):
        for r in tiles(reach):
            for half, total in enumerate(cross(refs[1 - parity], r, lane)):
                layer(z, refs[parity], r, half, total)

    def runs(reach_of, zs):
        found = []
        for z in zs[: len(zs) // 2 * 2 : 2]:
            if found and up8(reach_of(z)) == up8(reach_of(found[-1][0])):
                found[-1].append(z)
            else:
                found.append([z])
        return found

    def reach(z):
        return 2 * (nz - 1) - z

    later = list(range(1, nz))
    for run in runs(reach, later):

        def pair(i, carry, run=run):
            z = run[0] + 2 * i
            forward(z, run[0] % 2, reach(run[0]))
            forward(z + 1, (run[0] + 1) % 2, reach(run[0] + 1))
            return carry

        lax.fori_loop(0, len(run), pair, 0)
    if len(later) % 2:
        forward(later[-1], later[-1] % 2, reach(later[-1]))

    send = pltpu.make_async_copy(printed, printed_out, sems.at[0])
    send.start()
    unpack_halo(plan, 1, above, below, cabove, cbelow, cmh, csh)

    def back(z, out, r, spreads):
        for half, spread in enumerate(spreads):
            adjoint = field((cot, cot_side), (cmh, csh), half, z, r)
            if spread is not None:
                adjoint = adjoint + slope[z, half, r : r + SUB, :] * spread
            out[half, SUB + r : SUB + r + SUB, :] = adjoint * weight[z, half, r : r + SUB, :]
            if half == 0 and inside(r):
                k = r - top
                gradient[z, k : k + SUB, :] = adjoint * da[z, k : k + SUB, :]

    for r in tiles(nz - 1):
        back(nz - 1, refs[(nz - 1) % 2], r, (None, None))

    def backward(z, parity, reach):
        for r in tiles(reach):
            back(z, refs[parity], r, cross(refs[1 - parity], r, lane))

    later = list(range(nz - 2, 0, -1))
    for run in runs(lambda z: z, later):

        def pair(i, carry, run=run):
            z = run[0] - 2 * i
            backward(z, run[0] % 2, run[0])
            backward(z - 1, (run[0] + 1) % 2, run[0] - 1)
            return carry

        lax.fori_loop(0, len(run), pair, 0)
    if len(later) % 2:
        backward(later[-1], later[-1] % 2, later[-1])

    for r in range(top, top + rows, SUB):
        spread, _ = cross(odd, r, lane)
        k = r - top
        adjoint = cot[0, k : k + SUB, :] + slope[0, 0, r : r + SUB, :] * spread
        gradient[0, k : k + SUB, :] = adjoint * da[0, k : k + SUB, :]
    other = pltpu.make_async_copy(gradient, gradient_out, sems.at[1])
    other.start()
    send.wait()
    other.wait()


def near(x):
    return pltpu.with_memory_space_constraint(x, pltpu.VMEM)


def call(body, outs, *args, flops=100000):
    return pl.pallas_call(
        body,
        out_shape=[pltpu.VMEM(s, jnp.float32) for s in outs],
        in_specs=[VMEM] * len(args),
        out_specs=[VMEM] * len(outs),
        cost_estimate=pl.CostEstimate(flops=flops, bytes_accessed=flops, transcendentals=0),
        compiler_params=pltpu.CompilerParams(vmem_limit_bytes=4 << 20),
    )(*[near(x) for x in args])


def swap(axis, first, last):
    count = lax.axis_size(axis)
    forward = [(i, (i + 1) % count) for i in range(count)]
    backward = [(i, (i - 1) % count) for i in range(count)]
    return lax.ppermute(last, axis, forward), lax.ppermute(first, axis, backward)


def shards(density, cotangent):
    nz, rows, cols = density.shape
    plan = Plan(nz, rows, cols)
    part = functools.partial
    block = (nz, rows, cols)
    first, last = call(part(pack_rows, plan), [(plan.row_len, cols)] * 2, density, cotangent)
    above, below = swap("gx", first, last)
    first, last = call(part(pack_columns, plan), [(plan.col_tiles, rows, cols)] * 2, density, cotangent)
    left, right = swap("gy", first, last)
    first, last = call(part(pack_corners, plan), [(plan.corner_tiles, SUB, cols)] * 2, left, right)
    cabove, cbelow = swap("gx", first, last)
    sides = call(part(unpack_columns, plan), [block] * 2, left, right)
    full = rows + 2 * plan.halo
    halo = (nz, 2 * plan.halo, cols)
    work = (2, full + 2 * SUB, cols)
    scratch = [halo] * 4 + [work] * 2 + [(nz, 2, full, cols)] * 2 + [block] * 3
    args = (density, cotangent, *sides, above, below, cabove, cbelow)
    outs = pl.pallas_call(
        part(filter_body, plan),
        out_shape=[jax.ShapeDtypeStruct(block, jnp.float32)] * 2,
        in_specs=[VMEM] * len(args),
        out_specs=[pl.BlockSpec(memory_space=pltpu.HBM)] * 2,
        scratch_shapes=[pltpu.VMEM(s, jnp.float32) for s in scratch] + [pltpu.SemaphoreType.DMA((2,))],
        cost_estimate=pl.CostEstimate(flops=10000000, bytes_accessed=1000000, transcendentals=0),
        compiler_params=pltpu.CompilerParams(vmem_limit_bytes=24 << 20),
    )(*[near(x) for x in args])
    return tuple(outs)


def solution(mesh):
    placed = P(None, "gx", "gy")
    return jax.shard_map(
        shards,
        mesh=mesh,
        in_specs=(placed, placed),
        out_specs=(placed, placed),
        check_vma=False,
    )
```

```python
import functools
import math

import jax
import jax.numpy as jnp
from jax import lax
from jax.experimental import pallas as pl
from jax.experimental.pallas import tpu as pltpu
from jax.sharding import PartitionSpec as P

power_p = 20.0
root_q = 20.0 + math.log(5.0) / math.log(0.1)
smooth_eps = 0.0001
SUB = 8

VMEM = pl.BlockSpec(memory_space=pltpu.VMEM)


def up8(n):
    return -(-n // SUB) * SUB


class Plan:
    def __init__(self, layers, rows, cols):
        self.nz, self.rows, self.cols = layers, rows, cols
        self.fields = [(0, z, 2 * (layers - 1) - z) for z in range(layers)]
        self.fields += [(1, z, z) for z in range(layers - 1, 0, -1)]
        far = 2 * (layers - 1)
        self.halo = up8(far)
        self.row_at = {}
        at = SUB
        for arr, z, d in self.fields:
            self.row_at[arr, z] = at
            at += d
        self.row_len = up8(at) + SUB
        self.col_at, self.col_tiles = self.fit([((arr, z), d) for arr, z, d in self.fields])
        items = []
        for arr, z, d in self.fields:
            for k in range(-(-(d - 1) // SUB)):
                items.append(((arr, z, k), 2 * (d - 1 - SUB * k)))
        self.corner_at, self.corner_tiles = self.fit(items)

    def fit(self, items):
        room, where = [], {}
        for key, width in sorted(items, key=lambda item: -item[1]):
            for tile, used in enumerate(room):
                if used + width <= self.cols:
                    break
            else:
                tile = len(room)
                room.append(0)
            where[key] = (tile, room[tile])
            room[tile] += width
        return where, len(room)


def shift(x, amount):
    amount %= x.shape[1]
    return x if amount == 0 else pltpu.roll(x, amount, 1)


def lanes_of(shape):
    return lax.broadcasted_iota(jnp.int32, shape, 1)


def fetch(plan, dens_in, cot_in, dens, cot, first, last, sems):
    copies = [
        pltpu.make_async_copy(src, dst, sems.at[i])
        for i, (src, dst) in enumerate(((dens_in, dens), (cot_in, cot)))
    ]
    for copy in copies:
        copy.start()
    end = plan.row_at[1, 1] + 1
    for ref in (first, last):
        ref[:SUB, :] = jnp.zeros((SUB, plan.cols), jnp.float32)
        ref[end:, :] = jnp.zeros((plan.row_len - end, plan.cols), jnp.float32)
    for turn, copy in enumerate(copies):
        copy.wait()
        for arr, z, d in plan.fields:
            if arr == turn:
                src, at = (dens, cot)[arr], plan.row_at[arr, z]
                first[at : at + d, :] = src[z, :d, :]
                last[at : at + d, :] = src[z, plan.rows - d :, :]


def pack_columns(plan, dens, cot, first, last):
    n = plan.cols
    lane = lanes_of((SUB, n))
    for tile in range(plan.col_tiles):
        inside = [f for f in plan.fields if plan.col_at[f[0], f[1]][0] == tile]
        inside.sort(key=lambda f: plan.col_at[f[0], f[1]][1])
        for r in range(0, plan.rows, SUB):
            one, two = None, None
            for arr, z, d in inside:
                at = plan.col_at[arr, z][1]
                x = (dens, cot)[arr][z, r : r + SUB, :]
                a, b = shift(x, at), shift(x, at + d)
                if one is None:
                    one, two = a, b
                else:
                    here = lane >= at
                    one, two = jnp.where(here, a, one), jnp.where(here, b, two)
            first[tile, r : r + SUB, :] = one
            last[tile, r : r + SUB, :] = two


def pack_corners(plan, left, right, first, last):
    lane = lanes_of((SUB, plan.cols))
    out = [[None] * plan.corner_tiles, [None] * plan.corner_tiles]
    order = sorted(plan.corner_at.items(), key=lambda item: item[1][1])
    reach = {(arr, z): d for arr, z, d in plan.fields}
    for (arr, z, k), (tile, at) in order:
        d = reach[arr, z]
        w = d - 1 - SUB * k
        ctile, cat = plan.col_at[arr, z]
        for way in range(2):
            r = SUB * k if way == 0 else plan.rows - SUB * (k + 1)
            a = shift(left[ctile, r : r + SUB, :], at - (cat + d - w))
            b = shift(right[ctile, r : r + SUB, :], at + w - cat)
            both = jnp.where(lane >= at + w, b, a)
            prev = out[way][tile]
            out[way][tile] = both if prev is None else jnp.where(lane >= at, both, prev)
    for tile in range(plan.corner_tiles):
        first[tile] = out[0][tile]
        last[tile] = out[1][tile]


def unpack_columns(plan, left, right, *sides):
    n = plan.cols
    low = lanes_of((SUB, n)) < n // 2
    for arr, z, d in plan.fields:
        tile, at = plan.col_at[arr, z]
        for r in range(0, plan.rows, SUB):
            x = shift(left[tile, r : r + SUB, :], -(at + d))
            y = shift(right[tile, r : r + SUB, :], -at)
            sides[arr][z, r : r + SUB, :] = jnp.where(low, y, x)


def unpack_halo(plan, arr, above, below, cabove, cbelow, main, side):
    top = plan.halo
    for a, z, d in plan.fields:
        if a != arr:
            continue
        at = plan.row_at[arr, z]
        for k in range(-(-d // SUB)):
            lo, hi = top - SUB * (k + 1), top + SUB * k
            main[z, lo : lo + SUB, :] = above[at + d - SUB * (k + 1) : at + d - SUB * k, :]
            main[z, hi : hi + SUB, :] = below[at + SUB * k : at + SUB * (k + 1), :]
            w = d - 1 - SUB * k
            if w > 0:
                tile, cor = plan.corner_at[arr, z, k]
                side[z, lo : lo + SUB, :] = shift(cabove[tile], -(cor + w))
                side[z, hi : hi + SUB, :] = shift(cbelow[tile], -(cor + w))


def cross(ref, r, lane):
    n = lane.shape[1]
    b = SUB + r
    m, s = ref[0, b : b + SUB, :], ref[1, b : b + SUB, :]
    m1, s1 = pltpu.roll(m, 1, 1), pltpu.roll(s, 1, 1)
    m2, s2 = pltpu.roll(m, n - 1, 1), pltpu.roll(s, n - 1, 1)
    vm = m + ref[0, b - 1 : b + SUB - 1, :] + ref[0, b + 1 : b + SUB + 1, :]
    vs = s + ref[1, b - 1 : b + SUB - 1, :] + ref[1, b + 1 : b + SUB + 1, :]
    start, end = lane == 0, lane == n - 1
    hm = jnp.where(start, s1, m1) + jnp.where(end, s2, m2)
    hs = jnp.where(start, m1, s1) + jnp.where(end, m2, s2)
    return vm + hm, vs + hs


def filter_body(
    plan, dens, cot, dens_side, cot_side, above, below, cabove, cbelow,
    printed_out, gradient_out, dmh, dsh, cmh, csh, even, odd, slope, weight, da, printed, gradient, sems,
):
    nz, rows, n, top = plan.nz, plan.rows, plan.cols, plan.halo
    lane = lanes_of((SUB, n))
    full = top + rows + top
    unpack_halo(plan, 0, above, below, cabove, cbelow, dmh, dsh)

    margin = jnp.ones((SUB, n), jnp.float32)
    for ref in (even, odd):
        for half in range(2):
            ref[half, :SUB, :] = margin
            ref[half, SUB + full :, :] = margin

    def tiles(reach):
        depth = up8(max(reach, 0))
        return range(top - depth, top + rows + depth, SUB)

    def inside(r):
        return top <= r < top + rows

    def field(blocks, halos, half, z, r):
        if inside(r):
            return blocks[half][z, r - top : r - top + SUB, :]
        at = r if r < top else r - rows
        return halos[half][z, at : at + SUB, :]

    coef = up8(nz - 1)

    def layer(z, out, r, half, total):
        density = field((dens, dens_side), (dmh, dsh), half, z, r)
        if total is None:
            level = jnp.ones_like(density)
        else:
            lg = jnp.log(total)
            level = jnp.exp2(lg * jnp.float32(1.0 / (root_q * math.log(2.0))))
        diff = density - level
        square = diff * diff + smooth_eps
        inv = lax.rsqrt(square)
        value = 0.5 * (density + level - square * inv + math.sqrt(smooth_eps))
        p2 = value * value
        p4 = p2 * p2
        p16 = (p4 * p4) * (p4 * p4)
        out[half, SUB + r : SUB + r + SUB, :] = p16 * p4
        if top - coef <= r < top + rows + coef:
            hu = 0.5 * (diff * inv)
            slope[z, half, r : r + SUB, :] = jnp.float32(power_p / root_q) * (p16 * (p2 * value))
            if total is not None:
                ratio = jnp.exp2(lg * jnp.float32((1.0 / root_q - 1.0) / math.log(2.0)))
                weight[z, half, r : r + SUB, :] = (0.5 + hu) * ratio
            if half == 0 and inside(r):
                printed[z, r - top : r - top + SUB, :] = value
                da[z, r - top : r - top + SUB, :] = 0.5 - hu

    for r in tiles(2 * (nz - 1)):
        for half in range(2):
            layer(0, even, r, half, None)

    refs = (even, odd)

    def forward(z, parity, reach):
        for r in tiles(reach):
            for half, total in enumerate(cross(refs[1 - parity], r, lane)):
                layer(z, refs[parity], r, half, total)

    def runs(reach_of, zs):
        found = []
        for z in zs[: len(zs) // 2 * 2 : 2]:
            if found and up8(reach_of(z)) == up8(reach_of(found[-1][0])):
                found[-1].append(z)
            else:
                found.append([z])
        return found

    def reach(z):
        return 2 * (nz - 1) - z

    later = list(range(1, nz))
    for run in runs(reach, later):

        def pair(i, carry, run=run):
            z = run[0] + 2 * i
            forward(z, run[0] % 2, reach(run[0]))
            forward(z + 1, (run[0] + 1) % 2, reach(run[0] + 1))
            return carry

        lax.fori_loop(0, len(run), pair, 0)
    if len(later) % 2:
        forward(later[-1], later[-1] % 2, reach(later[-1]))

    send = pltpu.make_async_copy(printed, printed_out, sems.at[0])
    send.start()
    unpack_halo(plan, 1, above, below, cabove, cbelow, cmh, csh)

    def back(z, out, r, spreads):
        for half, spread in enumerate(spreads):
            adjoint = field((cot, cot_side), (cmh, csh), half, z, r)
            if spread is not None:
                adjoint = adjoint + slope[z, half, r : r + SUB, :] * spread
            out[half, SUB + r : SUB + r + SUB, :] = adjoint * weight[z, half, r : r + SUB, :]
            if half == 0 and inside(r):
                k = r - top
                gradient[z, k : k + SUB, :] = adjoint * da[z, k : k + SUB, :]

    for r in tiles(nz - 1):
        back(nz - 1, refs[(nz - 1) % 2], r, (None, None))

    def backward(z, parity, reach):
        for r in tiles(reach):
            back(z, refs[parity], r, cross(refs[1 - parity], r, lane))

    later = list(range(nz - 2, 0, -1))
    for run in runs(lambda z: z, later):

        def pair(i, carry, run=run):
            z = run[0] - 2 * i
            backward(z, run[0] % 2, run[0])
            backward(z - 1, (run[0] + 1) % 2, run[0] - 1)
            return carry

        lax.fori_loop(0, len(run), pair, 0)
    if len(later) % 2:
        backward(later[-1], later[-1] % 2, later[-1])

    for r in range(top, top + rows, SUB):
        spread, _ = cross(odd, r, lane)
        k = r - top
        adjoint = cot[0, k : k + SUB, :] + slope[0, 0, r : r + SUB, :] * spread
        gradient[0, k : k + SUB, :] = adjoint * da[0, k : k + SUB, :]
    other = pltpu.make_async_copy(gradient, gradient_out, sems.at[1])
    other.start()
    send.wait()
    other.wait()


def near(x):
    return pltpu.with_memory_space_constraint(x, pltpu.VMEM)


def call(body, outs, *args, flops=100000):
    return pl.pallas_call(
        body,
        out_shape=[pltpu.VMEM(s, jnp.float32) for s in outs],
        in_specs=[VMEM] * len(args),
        out_specs=[VMEM] * len(outs),
        cost_estimate=pl.CostEstimate(flops=flops, bytes_accessed=flops, transcendentals=0),
        compiler_params=pltpu.CompilerParams(vmem_limit_bytes=4 << 20),
    )(*[near(x) for x in args])


def swap(axis, first, last):
    count = lax.axis_size(axis)
    forward = [(i, (i + 1) % count) for i in range(count)]
    backward = [(i, (i - 1) % count) for i in range(count)]
    return lax.ppermute(last, axis, forward), lax.ppermute(first, axis, backward)


def shards(density, cotangent):
    nz, rows, cols = density.shape
    plan = Plan(nz, rows, cols)
    part = functools.partial
    block = (nz, rows, cols)
    packed = (plan.row_len, cols)
    density, cotangent, first, last = pl.pallas_call(
        part(fetch, plan),
        out_shape=[pltpu.VMEM(s, jnp.float32) for s in (block, block, packed, packed)],
        in_specs=[pl.BlockSpec(memory_space=pltpu.HBM)] * 2,
        out_specs=[VMEM] * 4,
        scratch_shapes=[pltpu.SemaphoreType.DMA((2,))],
        cost_estimate=pl.CostEstimate(flops=100000, bytes_accessed=1000000, transcendentals=0),
        compiler_params=pltpu.CompilerParams(vmem_limit_bytes=4 << 20),
    )(*[pltpu.with_memory_space_constraint(x, pltpu.HBM) for x in (density, cotangent)])
    above, below = swap("gx", first, last)
    first, last = call(part(pack_columns, plan), [(plan.col_tiles, rows, cols)] * 2, density, cotangent)
    left, right = swap("gy", first, last)
    first, last = call(part(pack_corners, plan), [(plan.corner_tiles, SUB, cols)] * 2, left, right)
    cabove, cbelow = swap("gx", first, last)
    sides = call(part(unpack_columns, plan), [block] * 2, left, right)
    full = rows + 2 * plan.halo
    halo = (nz, 2 * plan.halo, cols)
    work = (2, full + 2 * SUB, cols)
    scratch = [halo] * 4 + [work] * 2 + [(nz, 2, full, cols)] * 2 + [block] * 3
    args = (density, cotangent, *sides, above, below, cabove, cbelow)
    outs = pl.pallas_call(
        part(filter_body, plan),
        out_shape=[jax.ShapeDtypeStruct(block, jnp.float32)] * 2,
        in_specs=[VMEM] * len(args),
        out_specs=[pl.BlockSpec(memory_space=pltpu.HBM)] * 2,
        scratch_shapes=[pltpu.VMEM(s, jnp.float32) for s in scratch] + [pltpu.SemaphoreType.DMA((2,))],
        cost_estimate=pl.CostEstimate(flops=10000000, bytes_accessed=1000000, transcendentals=0),
        compiler_params=pltpu.CompilerParams(vmem_limit_bytes=24 << 20),
    )(*[near(x) for x in args])
    return tuple(outs)


def solution(mesh):
    placed = P(None, "gx", "gy")
    return jax.shard_map(
        shards,
        mesh=mesh,
        in_specs=(placed, placed),
        out_specs=(placed, placed),
        check_vma=False,
    )
```

```python
import functools
import math

import jax
import jax.numpy as jnp
from jax import lax
from jax.experimental import pallas as pl
from jax.experimental.pallas import tpu as pltpu
from jax.sharding import PartitionSpec as P

power_p = 20.0
root_q = 20.0 + math.log(5.0) / math.log(0.1)
smooth_eps = 0.0001
SUB = 8

VMEM = pl.BlockSpec(memory_space=pltpu.VMEM)


def up8(n):
    return -(-n // SUB) * SUB


class Plan:
    def __init__(self, layers, rows, cols):
        self.nz, self.rows, self.cols = layers, rows, cols
        self.fields = [(0, z, 2 * (layers - 1) - z) for z in range(layers)]
        self.fields += [(1, z, z) for z in range(layers - 1, 0, -1)]
        far = 2 * (layers - 1)
        self.halo = up8(far)
        self.row_at = {}
        at = SUB
        for arr, z, d in self.fields:
            self.row_at[arr, z] = at
            at += d
        self.row_len = up8(at) + SUB
        self.col_at, self.col_tiles = self.fit([((arr, z), d) for arr, z, d in self.fields])
        items = []
        for arr, z, d in self.fields:
            for k in range(-(-(d - 1) // SUB)):
                items.append(((arr, z, k), 2 * (d - 1 - SUB * k)))
        self.corner_at, self.corner_tiles = self.fit(items)

    def fit(self, items):
        room, where = [], {}
        for key, width in sorted(items, key=lambda item: -item[1]):
            for tile, used in enumerate(room):
                if used + width <= self.cols:
                    break
            else:
                tile = len(room)
                room.append(0)
            where[key] = (tile, room[tile])
            room[tile] += width
        return where, len(room)


def shift(x, amount):
    amount %= x.shape[1]
    return x if amount == 0 else pltpu.roll(x, amount, 1)


def lanes_of(shape):
    return lax.broadcasted_iota(jnp.int32, shape, 1)


def fetch(plan, dens_in, cot_in, dens, cot, first, last, sems):
    copies = [
        pltpu.make_async_copy(src, dst, sems.at[i])
        for i, (src, dst) in enumerate(((dens_in, dens), (cot_in, cot)))
    ]
    for copy in copies:
        copy.start()
    end = plan.row_at[1, 1] + 1
    for ref in (first, last):
        ref[:SUB, :] = jnp.zeros((SUB, plan.cols), jnp.float32)
        ref[end:, :] = jnp.zeros((plan.row_len - end, plan.cols), jnp.float32)
    for turn, copy in enumerate(copies):
        copy.wait()
        for arr, z, d in plan.fields:
            if arr == turn:
                src, at = (dens, cot)[arr], plan.row_at[arr, z]
                first[at : at + d, :] = src[z, :d, :]
                last[at : at + d, :] = src[z, plan.rows - d :, :]


def pack_columns(plan, dens, cot, first, last):
    n = plan.cols
    lane = lanes_of((SUB, n))
    for tile in range(plan.col_tiles):
        inside = [f for f in plan.fields if plan.col_at[f[0], f[1]][0] == tile]
        inside.sort(key=lambda f: plan.col_at[f[0], f[1]][1])
        for r in range(0, plan.rows, SUB):
            one, two = None, None
            for arr, z, d in inside:
                at = plan.col_at[arr, z][1]
                x = (dens, cot)[arr][z, r : r + SUB, :]
                a, b = shift(x, at), shift(x, at + d)
                if one is None:
                    one, two = a, b
                else:
                    here = lane >= at
                    one, two = jnp.where(here, a, one), jnp.where(here, b, two)
            first[tile, r : r + SUB, :] = one
            last[tile, r : r + SUB, :] = two


def pack_corners(plan, left, right, first, last):
    lane = lanes_of((SUB, plan.cols))
    out = [[None] * plan.corner_tiles, [None] * plan.corner_tiles]
    order = sorted(plan.corner_at.items(), key=lambda item: item[1][1])
    reach = {(arr, z): d for arr, z, d in plan.fields}
    for (arr, z, k), (tile, at) in order:
        d = reach[arr, z]
        w = d - 1 - SUB * k
        ctile, cat = plan.col_at[arr, z]
        for way in range(2):
            r = SUB * k if way == 0 else plan.rows - SUB * (k + 1)
            a = shift(left[ctile, r : r + SUB, :], at - (cat + d - w))
            b = shift(right[ctile, r : r + SUB, :], at + w - cat)
            both = jnp.where(lane >= at + w, b, a)
            prev = out[way][tile]
            out[way][tile] = both if prev is None else jnp.where(lane >= at, both, prev)
    for tile in range(plan.corner_tiles):
        first[tile] = out[0][tile]
        last[tile] = out[1][tile]


def cross(ref, z, r, lane):
    n = lane.shape[1]
    b = SUB + r
    m, s = ref[z, 0, b : b + SUB, :], ref[z, 1, b : b + SUB, :]
    m1, s1 = pltpu.roll(m, 1, 1), pltpu.roll(s, 1, 1)
    m2, s2 = pltpu.roll(m, n - 1, 1), pltpu.roll(s, n - 1, 1)
    vm = m + ref[z, 0, b - 1 : b + SUB - 1, :] + ref[z, 0, b + 1 : b + SUB + 1, :]
    vs = s + ref[z, 1, b - 1 : b + SUB - 1, :] + ref[z, 1, b + 1 : b + SUB + 1, :]
    start, end = lane == 0, lane == n - 1
    hm = jnp.where(start, s1, m1) + jnp.where(end, s2, m2)
    hs = jnp.where(start, m1, s1) + jnp.where(end, m2, s2)
    return vm + hm, vs + hs


def layer(plan, z, r, half, density, total, power, slope, weight, da, printed):
    top, rows, coef = plan.halo, plan.rows, up8(z)
    if total is None:
        level = jnp.ones_like(density)
    else:
        lg = jnp.log(total)
        level = jnp.exp2(lg * jnp.float32(1.0 / (root_q * math.log(2.0))))
    diff = density - level
    square = diff * diff + smooth_eps
    inv = lax.rsqrt(square)
    value = 0.5 * (density + level - square * inv + math.sqrt(smooth_eps))
    p2 = value * value
    p4 = p2 * p2
    p16 = (p4 * p4) * (p4 * p4)
    if z < plan.nz - 1:
        power[z, half, SUB + r : SUB + r + SUB, :] = p16 * p4
    if top - coef <= r < top + rows + coef:
        u = diff * inv
        if z > 0 or half == 0:
            slope[z, half, r : r + SUB, :] = jnp.float32(0.5 * power_p / root_q) * (p16 * (p2 * value))
        if z > 0:
            ratio = jnp.exp2(lg * jnp.float32((1.0 / root_q - 1.0) / math.log(2.0)))
            weight[z, half, r : r + SUB, :] = (1.0 + u) * ratio
        if half == 0 and top <= r < top + rows:
            printed[z, r - top : r - top + SUB, :] = value
            da[z, r - top : r - top + SUB, :] = 0.5 - 0.5 * u


def inner_body(plan, dens, left, right, dens_side, cot_side, power, slope, weight, da, printed):
    nz, rows, n, top = plan.nz, plan.rows, plan.cols, plan.halo
    lane = lanes_of((SUB, n))
    low = lane < n // 2
    sides = (dens_side, cot_side)
    for arr, z, d in plan.fields:
        tile, at = plan.col_at[arr, z]
        for r in range(0, rows, SUB):
            x = shift(left[tile, r : r + SUB, :], -(at + d))
            y = shift(right[tile, r : r + SUB, :], -at)
            sides[arr][z, r : r + SUB, :] = jnp.where(low, y, x)
    margin = jnp.ones((SUB, n), jnp.float32)
    out = (power, slope, weight, da, printed)
    for z in range(nz):
        if z < nz - 1:
            for half in range(2):
                for r in (0, top, SUB + top + rows, SUB + 2 * top + rows):
                    power[z, half, r : r + SUB, :] = margin
        skip = z // SUB * SUB
        for k in range(skip, rows - skip, SUB):
            total = (None, None) if z == 0 else cross(power, z - 1, top + k, lane)
            for half in range(2):
                density = (dens, dens_side)[half][z, k : k + SUB, :]
                layer(plan, z, top + k, half, density, total[half], *out)


def outer_body(
    plan, dens, cot, dens_side, cot_side, above, below, cabove, cbelow, power_in, slope_in, weight_in, da_in, printed_in,
    power, slope, weight, da, printed, gradient_out, printed_out, gradient, work, sems,
):
    nz, rows, n, top = plan.nz, plan.rows, plan.cols, plan.halo
    lane = lanes_of((SUB, n))
    full = top + rows + top
    reach = {(arr, z): d for arr, z, d in plan.fields}
    out = (power, slope, weight, da, printed)

    margin = jnp.ones((SUB, n), jnp.float32)
    for half in range(2):
        for now in range(2):
            work[now, half, :SUB, :] = margin
            work[now, half, SUB + full :, :] = margin

    def inside(r):
        return top <= r < top + rows

    def field(arr, z, r, half):
        if inside(r):
            blocks = ((dens, dens_side), (cot, cot_side))[arr]
            return blocks[half][z, r - top : r - top + SUB, :]
        d = reach[arr, z]
        before = r < top
        k = (top - r) // SUB - 1 if before else (r - top - rows) // SUB
        if half == 0:
            at = plan.row_at[arr, z]
            if before:
                return above[at + d - SUB * (k + 1) : at + d - SUB * k, :]
            return below[at + SUB * k : at + SUB * (k + 1), :]
        w = d - 1 - SUB * k
        if w <= 0:
            return jnp.ones((SUB, n), jnp.float32)
        tile, cor = plan.corner_at[arr, z, k]
        return shift((cabove if before else cbelow)[tile], -(cor + w))

    def tiles(depth):
        return range(top - up8(depth), top + rows + up8(depth), SUB)

    for z in range(nz):
        edge = up8(z)
        for r in tiles(2 * (nz - 1) - z):
            if top + edge <= r < top + rows - edge:
                continue
            total = (None, None) if z == 0 else cross(power, z - 1, r, lane)
            for half in range(2):
                layer(plan, z, r, half, field(0, z, r, half), total[half], *out)

    copies = [pltpu.make_async_copy(printed, printed_out, sems.at[nz])]
    copies[0].start()

    for z in range(nz - 1, -1, -1):
        for r in tiles(z):
            if z == nz - 1:
                spreads = (None, None)
            else:
                spreads = cross(work, (z + 1) % 2, r, lane)
            for half in range(2 if z > 0 else 1):
                adjoint = field(1, z, r, half) if z > 0 else cot[0, r - top : r - top + SUB, :]
                if spreads[half] is not None:
                    adjoint = adjoint + slope[z, half, r : r + SUB, :] * spreads[half]
                if z > 0:
                    work[z % 2, half, SUB + r : SUB + r + SUB, :] = adjoint * weight[z, half, r : r + SUB, :]
                if half == 0 and inside(r):
                    k = r - top
                    gradient[z, k : k + SUB, :] = adjoint * da[z, k : k + SUB, :]
        copies.append(pltpu.make_async_copy(gradient.at[z], gradient_out.at[z], sems.at[z]))
        copies[-1].start()
    for copy in copies:
        copy.wait()


def swap(axis, first, last):
    count = lax.axis_size(axis)
    forward = [(i, (i + 1) % count) for i in range(count)]
    backward = [(i, (i - 1) % count) for i in range(count)]
    return lax.ppermute(last, axis, forward), lax.ppermute(first, axis, backward)


def near(x):
    return pltpu.with_memory_space_constraint(x, pltpu.VMEM)


def call(body, outs, *args, flops=100000, limit=4):
    return pl.pallas_call(
        body,
        out_shape=[pltpu.VMEM(s, jnp.float32) for s in outs],
        in_specs=[VMEM] * len(args),
        out_specs=[VMEM] * len(outs),
        cost_estimate=pl.CostEstimate(flops=flops, bytes_accessed=flops, transcendentals=0),
        compiler_params=pltpu.CompilerParams(vmem_limit_bytes=limit << 20),
    )(*[near(x) for x in args])


def shards(density, cotangent):
    nz, rows, cols = density.shape
    plan = Plan(nz, rows, cols)
    part = functools.partial
    block = (nz, rows, cols)
    packed = (plan.row_len, cols)
    density, cotangent, first, last = pl.pallas_call(
        part(fetch, plan),
        out_shape=[pltpu.VMEM(s, jnp.float32) for s in (block, block, packed, packed)],
        in_specs=[pl.BlockSpec(memory_space=pltpu.HBM)] * 2,
        out_specs=[VMEM] * 4,
        scratch_shapes=[pltpu.SemaphoreType.DMA((2,))],
        cost_estimate=pl.CostEstimate(flops=100000, bytes_accessed=1000000, transcendentals=0),
        compiler_params=pltpu.CompilerParams(vmem_limit_bytes=4 << 20),
    )(*[pltpu.with_memory_space_constraint(x, pltpu.HBM) for x in (density, cotangent)])
    above, below = swap("gx", first, last)
    first, last = call(part(pack_columns, plan), [(plan.col_tiles, rows, cols)] * 2, density, cotangent)
    left, right = swap("gy", first, last)
    first, last = call(part(pack_corners, plan), [(plan.corner_tiles, SUB, cols)] * 2, left, right)
    cabove, cbelow = swap("gx", first, last)
    full = rows + 2 * plan.halo
    power = (nz - 1, 2, full + 2 * SUB, cols)
    coef = (nz, 2, full, cols)
    kept = [power, coef, coef, block, block]
    dens_side, cot_side, *state = call(part(inner_body, plan), [block] * 2 + kept, density, left, right, limit=8)
    args = (density, cotangent, dens_side, cot_side, above, below, cabove, cbelow, *state)
    *_, gradient, printed = pl.pallas_call(
        part(outer_body, plan),
        out_shape=[pltpu.VMEM(s, jnp.float32) for s in kept] + [jax.ShapeDtypeStruct(block, jnp.float32)] * 2,
        in_specs=[VMEM] * len(args),
        out_specs=[VMEM] * len(kept) + [pl.BlockSpec(memory_space=pltpu.HBM)] * 2,
        scratch_shapes=[
            pltpu.VMEM(block, jnp.float32),
            pltpu.VMEM((2, 2, full + 2 * SUB, cols), jnp.float32),
            pltpu.SemaphoreType.DMA((nz + 1,)),
        ],
        input_output_aliases={len(args) - len(kept) + i: i for i in range(len(kept))},
        cost_estimate=pl.CostEstimate(flops=10000000, bytes_accessed=1000000, transcendentals=0),
        compiler_params=pltpu.CompilerParams(vmem_limit_bytes=8 << 20),
    )(*[near(x) for x in args])
    return printed, gradient


def solution(mesh):
    placed = P(None, "gx", "gy")
    return jax.shard_map(
        shards,
        mesh=mesh,
        in_specs=(placed, placed),
        out_specs=(placed, placed),
        check_vma=False,
    )
```

```python
import functools
import math

import jax
import jax.numpy as jnp
from jax import lax
from jax.experimental import pallas as pl
from jax.experimental.pallas import tpu as pltpu
from jax.sharding import PartitionSpec as P


power_p = 20.0
root_q = 20.0 + math.log(5.0) / math.log(0.1)
smooth_eps = 0.0001
SUB = 8

VMEM = pl.BlockSpec(memory_space=pltpu.VMEM)


def up8(n):
    return -(-n // SUB) * SUB


class Plan:
    def __init__(self, layers, rows, cols):
        self.nz, self.rows, self.cols = layers, rows, cols
        self.fields = [(0, z, 2 * (layers - 1) - z) for z in range(layers)]
        self.fields += [(1, z, z) for z in range(layers - 1, 0, -1)]
        far = 2 * (layers - 1)
        self.halo = up8(far)
        line = sorted(self.fields, key=lambda f: f[2] % SUB != 0)
        even = sum(d % SUB == 0 for _, _, d in line)
        line = line[1:] + line[:1]
        line = line[even - 2 : even - 1] + line[: even - 2] + line[even - 1 :] if even >= 2 else line
        self.margin = 0 if even >= 2 else SUB
        self.row_at = {}
        at = self.margin
        for arr, z, d in line:
            self.row_at[arr, z] = at
            at += d
        self.row_end = at
        self.row_len = up8(at) + self.margin
        self.col_at, self.col_tiles = self.fit([((arr, z), d) for arr, z, d in self.fields])
        items = []
        for arr, z, d in self.fields:
            for k in range(-(-(d - 1) // SUB)):
                items.append(((arr, z, k), 2 * (d - 1 - SUB * k)))
        self.corner_at, self.corner_tiles = self.fit(items)

    def fit(self, items):
        room, where = [], {}
        for key, width in sorted(items, key=lambda item: -item[1]):
            for tile, used in enumerate(room):
                if used + width <= self.cols:
                    break
            else:
                tile = len(room)
                room.append(0)
            where[key] = (tile, room[tile])
            room[tile] += width
        return where, len(room)


def shift(x, amount):
    amount %= x.shape[1]
    return x if amount == 0 else pltpu.roll(x, amount, 1)


def lanes_of(shape):
    return lax.broadcasted_iota(jnp.int32, shape, 1)


def odd_on(axis):
    return lax.rem(lax.axis_index(axis), 2) == 1


def fetch(plan, dens_in, cot_in, dens, cot, ours, theirs, sems):
    copies = [
        pltpu.make_async_copy(src, dst, sems.at[i])
        for i, (src, dst) in enumerate(((dens_in, dens), (cot_in, cot)))
    ]
    for copy in copies:
        copy.start()
    odd = odd_on("gx")
    for ref in (ours, theirs):
        if plan.margin > 0:
            ref[: plan.margin, :] = jnp.zeros((plan.margin, plan.cols), jnp.float32)
        if plan.row_len > plan.row_end:
            ref[plan.row_end :, :] = jnp.zeros((plan.row_len - plan.row_end, plan.cols), jnp.float32)
    for turn, copy in enumerate(copies):
        copy.wait()
        for arr, z, d in plan.fields:
            if arr == turn:
                src, at = (dens, cot)[arr], plan.row_at[arr, z]
                one, two = src[z, :d, :], src[z, plan.rows - d :, :]
                ours[at : at + d, :] = jnp.where(odd, one, two)
                theirs[at : at + d, :] = jnp.where(odd, two, one)


def pack_columns(plan, dens, cot, ours, theirs):
    n = plan.cols
    odd = odd_on("gy")
    lane = lanes_of((SUB, n))
    for tile in range(plan.col_tiles):
        inside = [f for f in plan.fields if plan.col_at[f[0], f[1]][0] == tile]
        inside.sort(key=lambda f: plan.col_at[f[0], f[1]][1])
        for r in range(0, plan.rows, SUB):
            one, two = None, None
            for arr, z, d in inside:
                at = plan.col_at[arr, z][1]
                x = (dens, cot)[arr][z, r : r + SUB, :]
                a, b = shift(x, at), shift(x, at + d)
                if one is None:
                    one, two = a, b
                else:
                    here = lane >= at
                    one, two = jnp.where(here, a, one), jnp.where(here, b, two)
            ours[tile, r : r + SUB, :] = jnp.where(odd, one, two)
            theirs[tile, r : r + SUB, :] = jnp.where(odd, two, one)


def pack_corners(plan, mine, other, ours, theirs):
    lane = lanes_of((SUB, plan.cols))
    odd_x, odd_y = odd_on("gx"), odd_on("gy")
    out = [[None] * plan.corner_tiles, [None] * plan.corner_tiles]
    order = sorted(plan.corner_at.items(), key=lambda item: item[1][1])
    reach = {(arr, z): d for arr, z, d in plan.fields}
    for (arr, z, k), (tile, at) in order:
        d = reach[arr, z]
        w = d - 1 - SUB * k
        ctile, cat = plan.col_at[arr, z]
        for way in range(2):
            r = SUB * k if way == 0 else plan.rows - SUB * (k + 1)
            x, y = mine[ctile, r : r + SUB, :], other[ctile, r : r + SUB, :]
            a = shift(jnp.where(odd_y, x, y), at - (cat + d - w))
            b = shift(jnp.where(odd_y, y, x), at + w - cat)
            both = jnp.where(lane >= at + w, b, a)
            prev = out[way][tile]
            out[way][tile] = both if prev is None else jnp.where(lane >= at, both, prev)
    for tile in range(plan.corner_tiles):
        ours[tile] = jnp.where(odd_x, out[0][tile], out[1][tile])
        theirs[tile] = jnp.where(odd_x, out[1][tile], out[0][tile])


def cross(ref, z, r, lane):
    n = lane.shape[1]
    b = SUB + r
    m, s = ref[z, 0, b : b + SUB, :], ref[z, 1, b : b + SUB, :]
    m1, s1 = pltpu.roll(m, 1, 1), pltpu.roll(s, 1, 1)
    m2, s2 = pltpu.roll(m, n - 1, 1), pltpu.roll(s, n - 1, 1)
    vm = m + ref[z, 0, b - 1 : b + SUB - 1, :] + ref[z, 0, b + 1 : b + SUB + 1, :]
    vs = s + ref[z, 1, b - 1 : b + SUB - 1, :] + ref[z, 1, b + 1 : b + SUB + 1, :]
    start, end = lane == 0, lane == n - 1
    hm = jnp.where(start, s1, m1) + jnp.where(end, s2, m2)
    hs = jnp.where(start, m1, s1) + jnp.where(end, m2, s2)
    return vm + hm, vs + hs


def layer(plan, z, r, half, density, total, power, slope, weight, da, printed):
    top, rows, coef = plan.halo, plan.rows, up8(z)
    if total is None:
        level = jnp.ones_like(density)
    else:
        lg = jnp.log(total)
        level = jnp.exp2(lg * jnp.float32(1.0 / (root_q * math.log(2.0))))
    diff = density - level
    square = diff * diff + smooth_eps
    inv = lax.rsqrt(square)
    value = 0.5 * (density + level - square * inv + math.sqrt(smooth_eps))
    p2 = value * value
    p4 = p2 * p2
    p16 = (p4 * p4) * (p4 * p4)
    if z < plan.nz - 1:
        power[z, half, SUB + r : SUB + r + SUB, :] = p16 * p4
    if top - coef <= r < top + rows + coef:
        u = diff * inv
        if z > 0 or half == 0:
            slope[z, half, r : r + SUB, :] = jnp.float32(0.5 * power_p / root_q) * (p16 * (p2 * value))
        if z > 0:
            ratio = jnp.exp2(lg * jnp.float32((1.0 / root_q - 1.0) / math.log(2.0)))
            weight[z, half, r : r + SUB, :] = (1.0 + u) * ratio
        if half == 0 and top <= r < top + rows:
            printed[z, r - top : r - top + SUB, :] = value
            da[z, r - top : r - top + SUB, :] = 0.5 - 0.5 * u


def inner_body(plan, dens, mine, other, dens_side, cot_side, power, slope, weight, da, printed):
    nz, rows, n, top = plan.nz, plan.rows, plan.cols, plan.halo
    lane = lanes_of((SUB, n))
    low = lane < n // 2
    sides = (dens_side, cot_side)
    odd = odd_on("gy")
    for arr, z, d in plan.fields:
        tile, at = plan.col_at[arr, z]
        for r in range(0, rows, SUB):
            x, y = mine[tile, r : r + SUB, :], other[tile, r : r + SUB, :]
            x, y = shift(jnp.where(odd, x, y), -(at + d)), shift(jnp.where(odd, y, x), -at)
            sides[arr][z, r : r + SUB, :] = jnp.where(low, y, x)
    margin = jnp.ones((SUB, n), jnp.float32)
    out = (power, slope, weight, da, printed)
    for z in range(nz):
        if z < nz - 1:
            for half in range(2):
                for r in (0, top, SUB + top + rows, SUB + 2 * top + rows):
                    power[z, half, r : r + SUB, :] = margin
        skip = z // SUB * SUB
        for k in range(skip, rows - skip, SUB):
            total = (None, None) if z == 0 else cross(power, z - 1, top + k, lane)
            for half in range(2):
                density = (dens, dens_side)[half][z, k : k + SUB, :]
                layer(plan, z, top + k, half, density, total[half], *out)


def outer_body(
    plan, dens, cot, dens_side, cot_side, mine, other, cmine, cother, power_in, slope_in, weight_in, da_in, printed_in,
    power, slope, weight, da, printed, gradient_out, printed_out, gradient, work, sems,
):
    nz, rows, n, top = plan.nz, plan.rows, plan.cols, plan.halo
    lane = lanes_of((SUB, n))
    full = top + rows + top
    reach = {(arr, z): d for arr, z, d in plan.fields}
    odd = odd_on("gx")
    out = (power, slope, weight, da, printed)

    margin = jnp.ones((SUB, n), jnp.float32)
    for half in range(2):
        for now in range(2):
            work[now, half, :SUB, :] = margin
            work[now, half, SUB + full :, :] = margin

    def inside(r):
        return top <= r < top + rows

    def field(arr, z, r, half):
        if inside(r):
            blocks = ((dens, dens_side), (cot, cot_side))[arr]
            return blocks[half][z, r - top : r - top + SUB, :]
        d = reach[arr, z]
        before = r < top
        k = (top - r) // SUB - 1 if before else (r - top - rows) // SUB
        if half == 0:
            at = plan.row_at[arr, z]
            at = at + d - SUB * (k + 1) if before else at + SUB * k
            x, y = mine[at : at + SUB, :], other[at : at + SUB, :]
            return jnp.where(odd, x, y) if before else jnp.where(odd, y, x)
        w = d - 1 - SUB * k
        if w <= 0:
            return jnp.ones((SUB, n), jnp.float32)
        tile, cor = plan.corner_at[arr, z, k]
        x, y = cmine[tile], cother[tile]
        return shift(jnp.where(odd, x, y) if before else jnp.where(odd, y, x), -(cor + w))

    def tiles(depth):
        return range(top - up8(depth), top + rows + up8(depth), SUB)

    for z in range(nz):
        edge = up8(z)
        for r in tiles(2 * (nz - 1) - z):
            if top + edge <= r < top + rows - edge:
                continue
            total = (None, None) if z == 0 else cross(power, z - 1, r, lane)
            for half in range(2):
                layer(plan, z, r, half, field(0, z, r, half), total[half], *out)

    copies = [pltpu.make_async_copy(printed, printed_out, sems.at[nz])]
    copies[0].start()

    for z in range(nz - 1, -1, -1):
        for r in tiles(z):
            if z == nz - 1:
                spreads = (None, None)
            else:
                spreads = cross(work, (z + 1) % 2, r, lane)
            for half in range(2 if z > 0 else 1):
                adjoint = field(1, z, r, half) if z > 0 else cot[0, r - top : r - top + SUB, :]
                if spreads[half] is not None:
                    adjoint = adjoint + slope[z, half, r : r + SUB, :] * spreads[half]
                if z > 0:
                    work[z % 2, half, SUB + r : SUB + r + SUB, :] = adjoint * weight[z, half, r : r + SUB, :]
                if half == 0 and inside(r):
                    k = r - top
                    gradient[z, k : k + SUB, :] = adjoint * da[z, k : k + SUB, :]
        copies.append(pltpu.make_async_copy(gradient.at[z], gradient_out.at[z], sems.at[z]))
        copies[-1].start()
    for copy in copies:
        copy.wait()


def swap(axis, ours, theirs):
    count = lax.axis_size(axis)
    assert count % 2 == 0
    results = []
    for turn, x in enumerate((ours, theirs)):
        ends = [((i + turn) % count, (i + turn + 1) % count) for i in range(0, count, 2)]
        results.append(lax.ppermute(x, axis, [p for a, b in ends for p in ((a, b), (b, a))]))
    return results


def near(x):
    return pltpu.with_memory_space_constraint(x, pltpu.VMEM)


def call(body, outs, *args, flops=100000, limit=4):
    return pl.pallas_call(
        body,
        out_shape=[pltpu.VMEM(s, jnp.float32) for s in outs],
        in_specs=[VMEM] * len(args),
        out_specs=[VMEM] * len(outs),
        cost_estimate=pl.CostEstimate(flops=flops, bytes_accessed=flops, transcendentals=0),
        compiler_params=pltpu.CompilerParams(vmem_limit_bytes=limit << 20),
    )(*[near(x) for x in args])


def shards(density, cotangent):
    nz, rows, cols = density.shape
    plan = Plan(nz, rows, cols)
    part = functools.partial
    block = (nz, rows, cols)
    packed = (plan.row_len, cols)
    density, cotangent, ours, theirs = pl.pallas_call(
        part(fetch, plan),
        out_shape=[pltpu.VMEM(s, jnp.float32) for s in (block, block, packed, packed)],
        in_specs=[pl.BlockSpec(memory_space=pltpu.HBM)] * 2,
        out_specs=[VMEM] * 4,
        scratch_shapes=[pltpu.SemaphoreType.DMA((2,))],
        cost_estimate=pl.CostEstimate(flops=100000, bytes_accessed=1000000, transcendentals=0),
        compiler_params=pltpu.CompilerParams(vmem_limit_bytes=4 << 20),
    )(*[pltpu.with_memory_space_constraint(x, pltpu.HBM) for x in (density, cotangent)])
    near_rows = swap("gx", ours, theirs)
    ours, theirs = call(part(pack_columns, plan), [(plan.col_tiles, rows, cols)] * 2, density, cotangent)
    sides = swap("gy", ours, theirs)
    ours, theirs = call(part(pack_corners, plan), [(plan.corner_tiles, SUB, cols)] * 2, *sides)
    corners = swap("gx", ours, theirs)
    full = rows + 2 * plan.halo
    power = (nz - 1, 2, full + 2 * SUB, cols)
    coef = (nz, 2, full, cols)
    kept = [power, coef, coef, block, block]
    dens_side, cot_side, *state = call(part(inner_body, plan), [block] * 2 + kept, density, *sides, limit=8)
    args = (density, cotangent, dens_side, cot_side, *near_rows, *corners, *state)
    *_, gradient, printed = pl.pallas_call(
        part(outer_body, plan),
        out_shape=[pltpu.VMEM(s, jnp.float32) for s in kept] + [jax.ShapeDtypeStruct(block, jnp.float32)] * 2,
        in_specs=[VMEM] * len(args),
        out_specs=[VMEM] * len(kept) + [pl.BlockSpec(memory_space=pltpu.HBM)] * 2,
        scratch_shapes=[
            pltpu.VMEM(block, jnp.float32),
            pltpu.VMEM((2, 2, full + 2 * SUB, cols), jnp.float32),
            pltpu.SemaphoreType.DMA((nz + 1,)),
        ],
        input_output_aliases={len(args) - len(kept) + i: i for i in range(len(kept))},
        cost_estimate=pl.CostEstimate(flops=10000000, bytes_accessed=1000000, transcendentals=0),
        compiler_params=pltpu.CompilerParams(vmem_limit_bytes=8 << 20),
    )(*[near(x) for x in args])
    return printed, gradient


def solution(mesh):
    placed = P(None, "gx", "gy")
    return jax.shard_map(
        shards,
        mesh=mesh,
        in_specs=(placed, placed),
        out_specs=(placed, placed),
        check_vma=False,
    )
```

```python
import functools
import math

import jax
import jax.numpy as jnp
from jax import lax
from jax.experimental import pallas as pl
from jax.experimental.pallas import tpu as pltpu
from jax.sharding import PartitionSpec as P


power_p = 20.0
root_q = 20.0 + math.log(5.0) / math.log(0.1)
smooth_eps = 0.0001
SUB = 8

VMEM = pl.BlockSpec(memory_space=pltpu.VMEM)


def up8(n):
    return -(-n // SUB) * SUB


class Plan:
    def __init__(self, layers, rows, cols):
        self.nz, self.rows, self.cols = layers, rows, cols
        self.fields = [(0, z, 2 * (layers - 1) - z) for z in range(layers)]
        self.fields += [(1, z, z) for z in range(layers - 1, 0, -1)]
        far = 2 * (layers - 1)
        self.halo = up8(far)
        line = sorted(self.fields, key=lambda f: f[2] % SUB != 0)
        even = sum(d % SUB == 0 for _, _, d in line)
        line = line[1:] + line[:1]
        line = line[even - 2 : even - 1] + line[: even - 2] + line[even - 1 :] if even >= 2 else line
        self.margin = 0 if even >= 2 else SUB
        self.row_at = {}
        at = self.margin
        for arr, z, d in line:
            self.row_at[arr, z] = at
            at += d
        self.row_end = at
        self.row_len = up8(at) + self.margin
        items = [((arr, z, r), d) for arr, z, d in self.fields for r in range(0, rows, SUB)]
        self.col_at, self.col_tiles = self.fit(items, both=True)
        items = []
        for arr, z, d in self.fields:
            for k in range(-(-(d - 1) // SUB)):
                items.append(((arr, z, k), 2 * (d - 1 - SUB * k)))
        self.corner_at, self.corner_tiles = self.fit(items)

    def fit(self, items, both=False):
        room, widest, where = [], [], {}
        for key, width in sorted(items, key=lambda item: -item[1]):
            for tile, used in enumerate(room):
                if used + (widest[tile] if both else width) <= self.cols:
                    break
            else:
                tile = len(room)
                room.append(0)
                widest.append(width)
            where[key] = (tile, room[tile])
            room[tile] += width
        return where, len(room)


def shift(x, amount):
    amount %= x.shape[1]
    return x if amount == 0 else pltpu.roll(x, amount, 1)


def lanes_of(shape):
    return lax.broadcasted_iota(jnp.int32, shape, 1)


def odd_on(axis):
    return lax.rem(lax.axis_index(axis), 2) == 1


def fetch(plan, dens_in, cot_in, dens, cot, ours, theirs, sems):
    copies = [
        pltpu.make_async_copy(src, dst, sems.at[i])
        for i, (src, dst) in enumerate(((dens_in, dens), (cot_in, cot)))
    ]
    for copy in copies:
        copy.start()
    odd = odd_on("gx")
    for ref in (ours, theirs):
        if plan.margin > 0:
            ref[: plan.margin, :] = jnp.zeros((plan.margin, plan.cols), jnp.float32)
        if plan.row_len > plan.row_end:
            ref[plan.row_end :, :] = jnp.zeros((plan.row_len - plan.row_end, plan.cols), jnp.float32)
    for turn, copy in enumerate(copies):
        copy.wait()
        for arr, z, d in plan.fields:
            if arr == turn:
                src, at = (dens, cot)[arr], plan.row_at[arr, z]
                one, two = src[z, :d, :], src[z, plan.rows - d :, :]
                ours[at : at + d, :] = jnp.where(odd, one, two)
                theirs[at : at + d, :] = jnp.where(odd, two, one)


def pack_columns(plan, dens, cot, ours, theirs):
    n = plan.cols
    odd = odd_on("gy")
    lane = lanes_of((SUB, n))
    reach = {(arr, z): d for arr, z, d in plan.fields}
    for tile in range(plan.col_tiles):
        inside = [(at, key) for key, (t, at) in plan.col_at.items() if t == tile]
        one, two = None, None
        for at, (arr, z, r) in sorted(inside):
            d = reach[arr, z]
            x = shift((dens, cot)[arr][z, r : r + SUB, :], at)
            one = x if one is None else jnp.where(lane >= at, x, one)
            two = x if two is None else jnp.where((lane >= at - d) & (lane < at), x, two)
        ours[tile] = jnp.where(odd, one, two)
        theirs[tile] = jnp.where(odd, two, one)


def merge(odd, mine, other, at):
    n = mine.shape[1]
    lane = lanes_of(mine.shape)
    after = (lane >= at) & (lane < at + n // 2) if at <= n // 2 else (lane >= at) | (lane < at - n // 2)
    return jnp.where(after != odd, mine, other)


def pack_corners(plan, mine, other, ours, theirs):
    lane = lanes_of((SUB, plan.cols))
    odd_x, odd_y = odd_on("gx"), odd_on("gy")
    out = [[None] * plan.corner_tiles, [None] * plan.corner_tiles]
    order = sorted(plan.corner_at.items(), key=lambda item: item[1][1])
    reach = {(arr, z): d for arr, z, d in plan.fields}
    for (arr, z, k), (tile, at) in order:
        d = reach[arr, z]
        w = d - 1 - SUB * k
        for way in range(2):
            r = SUB * k if way == 0 else plan.rows - SUB * (k + 1)
            ctile, cat = plan.col_at[arr, z, r]
            x = merge(odd_y, mine[ctile], other[ctile], cat)
            x = shift(x, at + w - cat)
            prev = out[way][tile]
            out[way][tile] = x if prev is None else jnp.where(lane >= at, x, prev)
    for tile in range(plan.corner_tiles):
        ours[tile] = jnp.where(odd_x, out[0][tile], out[1][tile])
        theirs[tile] = jnp.where(odd_x, out[1][tile], out[0][tile])


def cross(ref, z, r, lane):
    n = lane.shape[1]
    b = SUB + r
    m, s = ref[z, 0, b : b + SUB, :], ref[z, 1, b : b + SUB, :]
    m1, s1 = pltpu.roll(m, 1, 1), pltpu.roll(s, 1, 1)
    m2, s2 = pltpu.roll(m, n - 1, 1), pltpu.roll(s, n - 1, 1)
    vm = m + ref[z, 0, b - 1 : b + SUB - 1, :] + ref[z, 0, b + 1 : b + SUB + 1, :]
    vs = s + ref[z, 1, b - 1 : b + SUB - 1, :] + ref[z, 1, b + 1 : b + SUB + 1, :]
    start, end = lane == 0, lane == n - 1
    hm = jnp.where(start, s1, m1) + jnp.where(end, s2, m2)
    hs = jnp.where(start, m1, s1) + jnp.where(end, m2, s2)
    return vm + hm, vs + hs


def layer(plan, z, r, half, density, total, power, slope, weight, da, printed):
    top, rows, coef = plan.halo, plan.rows, up8(z)
    if total is None:
        level = jnp.ones_like(density)
    else:
        lg = jnp.log(total)
        level = jnp.exp2(lg * jnp.float32(1.0 / (root_q * math.log(2.0))))
    diff = density - level
    square = diff * diff + smooth_eps
    inv = lax.rsqrt(square)
    value = 0.5 * (density + level - square * inv + math.sqrt(smooth_eps))
    p2 = value * value
    p4 = p2 * p2
    p16 = (p4 * p4) * (p4 * p4)
    if z < plan.nz - 1:
        power[z, half, SUB + r : SUB + r + SUB, :] = p16 * p4
    if top - coef <= r < top + rows + coef:
        u = diff * inv
        if z > 0 or half == 0:
            slope[z, half, r : r + SUB, :] = jnp.float32(0.5 * power_p / root_q) * (p16 * (p2 * value))
        if z > 0:
            ratio = jnp.exp2(lg * jnp.float32((1.0 / root_q - 1.0) / math.log(2.0)))
            weight[z, half, r : r + SUB, :] = (1.0 + u) * ratio
        if half == 0 and top <= r < top + rows:
            printed[z, r - top : r - top + SUB, :] = value
            da[z, r - top : r - top + SUB, :] = 0.5 - 0.5 * u


def inner_body(plan, dens, mine, other, dens_side, cot_side, power, slope, weight, da, printed):
    nz, rows, n, top = plan.nz, plan.rows, plan.cols, plan.halo
    lane = lanes_of((SUB, n))
    sides = (dens_side, cot_side)
    odd = odd_on("gy")
    for arr, z, d in plan.fields:
        for r in range(0, rows, SUB):
            tile, at = plan.col_at[arr, z, r]
            x = merge(odd, mine[tile], other[tile], at)
            sides[arr][z, r : r + SUB, :] = shift(x, -at)
    margin = jnp.ones((SUB, n), jnp.float32)
    out = (power, slope, weight, da, printed)
    for z in range(nz):
        if z < nz - 1:
            for half in range(2):
                for r in (0, top, SUB + top + rows, SUB + 2 * top + rows):
                    power[z, half, r : r + SUB, :] = margin
        skip = z // SUB * SUB
        for k in range(skip, rows - skip, SUB):
            total = (None, None) if z == 0 else cross(power, z - 1, top + k, lane)
            for half in range(2):
                density = (dens, dens_side)[half][z, k : k + SUB, :]
                layer(plan, z, top + k, half, density, total[half], *out)


def outer_body(
    plan, dens, cot, dens_side, cot_side, mine, other, cmine, cother, power_in, slope_in, weight_in, da_in, printed_in,
    power, slope, weight, da, printed, gradient_out, printed_out, gradient, work, sems,
):
    nz, rows, n, top = plan.nz, plan.rows, plan.cols, plan.halo
    lane = lanes_of((SUB, n))
    full = top + rows + top
    reach = {(arr, z): d for arr, z, d in plan.fields}
    odd = odd_on("gx")
    out = (power, slope, weight, da, printed)

    margin = jnp.ones((SUB, n), jnp.float32)
    for half in range(2):
        for now in range(2):
            work[now, half, :SUB, :] = margin
            work[now, half, SUB + full :, :] = margin

    def inside(r):
        return top <= r < top + rows

    def field(arr, z, r, half):
        if inside(r):
            blocks = ((dens, dens_side), (cot, cot_side))[arr]
            return blocks[half][z, r - top : r - top + SUB, :]
        d = reach[arr, z]
        before = r < top
        k = (top - r) // SUB - 1 if before else (r - top - rows) // SUB
        if half == 0:
            at = plan.row_at[arr, z]
            at = at + d - SUB * (k + 1) if before else at + SUB * k
            x, y = mine[at : at + SUB, :], other[at : at + SUB, :]
            return jnp.where(odd, x, y) if before else jnp.where(odd, y, x)
        w = d - 1 - SUB * k
        if w <= 0:
            return jnp.ones((SUB, n), jnp.float32)
        tile, cor = plan.corner_at[arr, z, k]
        x, y = cmine[tile], cother[tile]
        return shift(jnp.where(odd, x, y) if before else jnp.where(odd, y, x), -(cor + w))

    def tiles(depth):
        return range(top - up8(depth), top + rows + up8(depth), SUB)

    for z in range(nz):
        edge = up8(z)
        for r in tiles(2 * (nz - 1) - z):
            if top + edge <= r < top + rows - edge:
                continue
            total = (None, None) if z == 0 else cross(power, z - 1, r, lane)
            for half in range(2):
                layer(plan, z, r, half, field(0, z, r, half), total[half], *out)

    copies = [pltpu.make_async_copy(printed, printed_out, sems.at[nz])]
    copies[0].start()

    for z in range(nz - 1, -1, -1):
        for r in tiles(z):
            if z == nz - 1:
                spreads = (None, None)
            else:
                spreads = cross(work, (z + 1) % 2, r, lane)
            for half in range(2 if z > 0 else 1):
                adjoint = field(1, z, r, half) if z > 0 else cot[0, r - top : r - top + SUB, :]
                if spreads[half] is not None:
                    adjoint = adjoint + slope[z, half, r : r + SUB, :] * spreads[half]
                if z > 0:
                    work[z % 2, half, SUB + r : SUB + r + SUB, :] = adjoint * weight[z, half, r : r + SUB, :]
                if half == 0 and inside(r):
                    k = r - top
                    gradient[z, k : k + SUB, :] = adjoint * da[z, k : k + SUB, :]
        copies.append(pltpu.make_async_copy(gradient.at[z], gradient_out.at[z], sems.at[z]))
        copies[-1].start()
    for copy in copies:
        copy.wait()


def swap(axis, ours, theirs):
    count = lax.axis_size(axis)
    assert count % 2 == 0
    results = []
    for turn, x in enumerate((ours, theirs)):
        ends = [((i + turn) % count, (i + turn + 1) % count) for i in range(0, count, 2)]
        results.append(lax.ppermute(x, axis, [p for a, b in ends for p in ((a, b), (b, a))]))
    return results


def near(x):
    return pltpu.with_memory_space_constraint(x, pltpu.VMEM)


def call(body, outs, *args, flops=100000, limit=4):
    return pl.pallas_call(
        body,
        out_shape=[pltpu.VMEM(s, jnp.float32) for s in outs],
        in_specs=[VMEM] * len(args),
        out_specs=[VMEM] * len(outs),
        cost_estimate=pl.CostEstimate(flops=flops, bytes_accessed=flops, transcendentals=0),
        compiler_params=pltpu.CompilerParams(vmem_limit_bytes=limit << 20),
    )(*[near(x) for x in args])


def shards(density, cotangent):
    nz, rows, cols = density.shape
    plan = Plan(nz, rows, cols)
    part = functools.partial
    block = (nz, rows, cols)
    packed = (plan.row_len, cols)
    density, cotangent, ours, theirs = pl.pallas_call(
        part(fetch, plan),
        out_shape=[pltpu.VMEM(s, jnp.float32) for s in (block, block, packed, packed)],
        in_specs=[pl.BlockSpec(memory_space=pltpu.HBM)] * 2,
        out_specs=[VMEM] * 4,
        scratch_shapes=[pltpu.SemaphoreType.DMA((2,))],
        cost_estimate=pl.CostEstimate(flops=100000, bytes_accessed=1000000, transcendentals=0),
        compiler_params=pltpu.CompilerParams(vmem_limit_bytes=4 << 20),
    )(*[pltpu.with_memory_space_constraint(x, pltpu.HBM) for x in (density, cotangent)])
    near_rows = swap("gx", ours, theirs)
    ours, theirs = call(part(pack_columns, plan), [(plan.col_tiles, SUB, cols)] * 2, density, cotangent)
    sides = swap("gy", ours, theirs)
    ours, theirs = call(part(pack_corners, plan), [(plan.corner_tiles, SUB, cols)] * 2, *sides)
    corners = swap("gx", ours, theirs)
    full = rows + 2 * plan.halo
    power = (nz - 1, 2, full + 2 * SUB, cols)
    coef = (nz, 2, full, cols)
    kept = [power, coef, coef, block, block]
    dens_side, cot_side, *state = call(part(inner_body, plan), [block] * 2 + kept, density, *sides, limit=8)
    args = (density, cotangent, dens_side, cot_side, *near_rows, *corners, *state)
    *_, gradient, printed = pl.pallas_call(
        part(outer_body, plan),
        out_shape=[pltpu.VMEM(s, jnp.float32) for s in kept] + [jax.ShapeDtypeStruct(block, jnp.float32)] * 2,
        in_specs=[VMEM] * len(args),
        out_specs=[VMEM] * len(kept) + [pl.BlockSpec(memory_space=pltpu.HBM)] * 2,
        scratch_shapes=[
            pltpu.VMEM(block, jnp.float32),
            pltpu.VMEM((2, 2, full + 2 * SUB, cols), jnp.float32),
            pltpu.SemaphoreType.DMA((nz + 1,)),
        ],
        input_output_aliases={len(args) - len(kept) + i: i for i in range(len(kept))},
        cost_estimate=pl.CostEstimate(flops=10000000, bytes_accessed=1000000, transcendentals=0),
        compiler_params=pltpu.CompilerParams(vmem_limit_bytes=8 << 20),
    )(*[near(x) for x in args])
    return printed, gradient


def solution(mesh):
    placed = P(None, "gx", "gy")
    return jax.shard_map(
        shards,
        mesh=mesh,
        in_specs=(placed, placed),
        out_specs=(placed, placed),
        check_vma=False,
    )
```

```python
import functools
import math

import jax
import jax.numpy as jnp
from jax import lax
from jax.experimental import pallas as pl
from jax.experimental.pallas import tpu as pltpu
from jax.sharding import PartitionSpec as P


power_p = 20.0
root_q = 20.0 + math.log(5.0) / math.log(0.1)
smooth_eps = 0.0001
SUB = 8

VMEM = pl.BlockSpec(memory_space=pltpu.VMEM)


def up8(n):
    return -(-n // SUB) * SUB


class Plan:
    def __init__(self, layers, rows, cols):
        self.nz, self.rows, self.cols = layers, rows, cols
        self.fields = [(0, z, 2 * (layers - 1) - z) for z in range(layers)]
        self.fields += [(1, z, z) for z in range(layers - 1, 0, -1)]
        far = 2 * (layers - 1)
        self.halo = up8(far)
        line = sorted(self.fields, key=lambda f: f[2] % SUB != 0)
        even = sum(d % SUB == 0 for _, _, d in line)
        line = line[1:] + line[:1]
        line = line[even - 2 : even - 1] + line[: even - 2] + line[even - 1 :] if even >= 2 else line
        self.margin = 0 if even >= 2 else SUB
        self.row_at = {}
        at = self.margin
        for arr, z, d in line:
            self.row_at[arr, z] = at
            at += d
        self.row_end = at
        self.row_len = up8(at) + self.margin
        items = [((arr, z, r), d) for arr, z, d in self.fields for r in range(0, rows, SUB)]
        self.col_at, self.col_tiles = self.fit(items, both=True)
        items = []
        for arr, z, d in self.fields:
            for k in range(-(-(d - 1) // SUB)):
                for half in range(2):
                    if (w := self.corner_width(d, k, half)) > 0:
                        items.append(((arr, z, k, half), 2 * w))
        self.corner_at, bins = self.fit(items)
        self.corner_tiles = -(-bins // 2)

    def corner_width(self, d, k, half):
        return d - 1 - SUB * k - SUB // 2 * half

    def fit(self, items, both=False):
        room, widest, where = [], [], {}
        for key, width in sorted(items, key=lambda item: -item[1]):
            for tile, used in enumerate(room):
                if used + (widest[tile] if both else width) <= self.cols:
                    break
            else:
                tile = len(room)
                room.append(0)
                widest.append(width)
            where[key] = (tile, room[tile])
            room[tile] += width
        return where, len(room)


def shift(x, amount):
    amount %= x.shape[1]
    return x if amount == 0 else pltpu.roll(x, amount, 1)


def lanes_of(shape):
    return lax.broadcasted_iota(jnp.int32, shape, 1)


def odd_on(axis):
    return lax.rem(lax.axis_index(axis), 2) == 1


def fetch(plan, dens_in, cot_in, dens, cot, ours, theirs, sems):
    copies = [
        pltpu.make_async_copy(src, dst, sems.at[i])
        for i, (src, dst) in enumerate(((dens_in, dens), (cot_in, cot)))
    ]
    for copy in copies:
        copy.start()
    odd = odd_on("gx")
    for ref in (ours, theirs):
        if plan.margin > 0:
            ref[: plan.margin, :] = jnp.zeros((plan.margin, plan.cols), jnp.float32)
        if plan.row_len > plan.row_end:
            ref[plan.row_end :, :] = jnp.zeros((plan.row_len - plan.row_end, plan.cols), jnp.float32)
    for turn, copy in enumerate(copies):
        copy.wait()
        for arr, z, d in plan.fields:
            if arr == turn:
                src, at = (dens, cot)[arr], plan.row_at[arr, z]
                one, two = src[z, :d, :], src[z, plan.rows - d :, :]
                ours[at : at + d, :] = jnp.where(odd, one, two)
                theirs[at : at + d, :] = jnp.where(odd, two, one)


def pack_columns(plan, dens, cot, ours, theirs):
    n = plan.cols
    odd = odd_on("gy")
    lane = lanes_of((SUB, n))
    reach = {(arr, z): d for arr, z, d in plan.fields}
    for tile in range(plan.col_tiles):
        inside = [(at, key) for key, (t, at) in plan.col_at.items() if t == tile]
        one, two = None, None
        for at, (arr, z, r) in sorted(inside):
            d = reach[arr, z]
            x = shift((dens, cot)[arr][z, r : r + SUB, :], at)
            one = x if one is None else jnp.where(lane >= at, x, one)
            two = x if two is None else jnp.where((lane >= at - d) & (lane < at), x, two)
        ours[tile] = jnp.where(odd, one, two)
        theirs[tile] = jnp.where(odd, two, one)


def merge(odd, mine, other, at):
    n = mine.shape[1]
    lane = lanes_of(mine.shape)
    after = (lane >= at) & (lane < at + n // 2) if at <= n // 2 else (lane >= at) | (lane < at - n // 2)
    return jnp.where(after != odd, mine, other)


def pack_corners(plan, mine, other, ours, theirs):
    lane = lanes_of((SUB, plan.cols))
    odd_x, odd_y = odd_on("gx"), odd_on("gy")
    bins = 2 * plan.corner_tiles
    out = [[jnp.zeros(lane.shape, jnp.float32)] * bins, [jnp.zeros(lane.shape, jnp.float32)] * bins]
    reach = {(arr, z): d for arr, z, d in plan.fields}
    for (arr, z, k, half), (place, at) in sorted(plan.corner_at.items(), key=lambda item: item[1][1]):
        w = plan.corner_width(reach[arr, z], k, half)
        for way in range(2):
            r = SUB * k if way == 0 else plan.rows - SUB * (k + 1)
            ctile, cat = plan.col_at[arr, z, r]
            x = merge(odd_y, mine[ctile], other[ctile], cat)
            x = turn(shift(x, at + w - cat), half != way, place % 2)
            out[way][place] = x if at == 0 else jnp.where(lane >= at, x, out[way][place])
    low = lax.broadcasted_iota(jnp.int32, lane.shape, 0) < SUB // 2
    for tile in range(plan.corner_tiles):
        one, two = [jnp.where(low, out[way][2 * tile], out[way][2 * tile + 1]) for way in range(2)]
        ours[tile] = jnp.where(odd_x, one, two)
        theirs[tile] = jnp.where(odd_x, two, one)


def turn(x, src, dst):
    return x if bool(src) == bool(dst) else pltpu.roll(x, SUB // 2, 0)


def cross(ref, z, r, lane):
    n = lane.shape[1]
    b = SUB + r
    m, s = ref[z, 0, b : b + SUB, :], ref[z, 1, b : b + SUB, :]
    m1, s1 = pltpu.roll(m, 1, 1), pltpu.roll(s, 1, 1)
    m2, s2 = pltpu.roll(m, n - 1, 1), pltpu.roll(s, n - 1, 1)
    vm = m + ref[z, 0, b - 1 : b + SUB - 1, :] + ref[z, 0, b + 1 : b + SUB + 1, :]
    vs = s + ref[z, 1, b - 1 : b + SUB - 1, :] + ref[z, 1, b + 1 : b + SUB + 1, :]
    start, end = lane == 0, lane == n - 1
    hm = jnp.where(start, s1, m1) + jnp.where(end, s2, m2)
    hs = jnp.where(start, m1, s1) + jnp.where(end, m2, s2)
    return vm + hm, vs + hs


def layer(plan, z, r, half, density, total, power, slope, weight, da, printed):
    top, rows, coef = plan.halo, plan.rows, up8(z)
    if total is None:
        level = jnp.ones_like(density)
    else:
        lg = lax.log2(total)
        level = jnp.exp2(lg * jnp.float32(1.0 / root_q))
    diff = density - level
    square = diff * diff + smooth_eps
    inv = lax.rsqrt(square)
    value = 0.5 * (density + level - square * inv + math.sqrt(smooth_eps))
    p2 = value * value
    p4 = p2 * p2
    p16 = (p4 * p4) * (p4 * p4)
    if z < plan.nz - 1:
        power[z, half, SUB + r : SUB + r + SUB, :] = p16 * p4
    if top - coef <= r < top + rows + coef:
        u = diff * inv
        if z > 0 or half == 0:
            slope[z, half, r : r + SUB, :] = jnp.float32(0.5 * power_p / root_q) * (p16 * (p2 * value))
        if z > 0:
            ratio = jnp.exp2(lg * jnp.float32(1.0 / root_q - 1.0))
            weight[z, half, r : r + SUB, :] = (1.0 + u) * ratio
        if half == 0 and top <= r < top + rows:
            printed[z, r - top : r - top + SUB, :] = value
            da[z, r - top : r - top + SUB, :] = 0.5 - 0.5 * u


def inner_body(plan, dens, mine, other, dens_side, cot_side, power, slope, weight, da, printed):
    nz, rows, n, top = plan.nz, plan.rows, plan.cols, plan.halo
    lane = lanes_of((SUB, n))
    sides = (dens_side, cot_side)
    odd = odd_on("gy")
    for arr, z, d in plan.fields:
        for r in range(0, rows, SUB):
            tile, at = plan.col_at[arr, z, r]
            x = merge(odd, mine[tile], other[tile], at)
            sides[arr][z, r : r + SUB, :] = shift(x, -at)
    margin = jnp.ones((SUB, n), jnp.float32)
    out = (power, slope, weight, da, printed)
    for z in range(nz):
        if z < nz - 1:
            for half in range(2):
                for r in (0, top, SUB + top + rows, SUB + 2 * top + rows):
                    power[z, half, r : r + SUB, :] = margin
        skip = z // SUB * SUB
        for k in range(skip, rows - skip, SUB):
            total = (None, None) if z == 0 else cross(power, z - 1, top + k, lane)
            for half in range(2):
                density = (dens, dens_side)[half][z, k : k + SUB, :]
                layer(plan, z, top + k, half, density, total[half], *out)


def outer_body(
    plan, dens, cot, dens_side, cot_side, mine, other, cmine, cother, power_in, slope_in, weight_in, da_in, printed_in,
    power, slope, weight, da, printed, gradient_out, printed_out, gradient, work, sems,
):
    nz, rows, n, top = plan.nz, plan.rows, plan.cols, plan.halo
    lane = lanes_of((SUB, n))
    low = lax.broadcasted_iota(jnp.int32, lane.shape, 0) < SUB // 2
    full = top + rows + top
    reach = {(arr, z): d for arr, z, d in plan.fields}
    odd = odd_on("gx")
    out = (power, slope, weight, da, printed)

    margin = jnp.ones((SUB, n), jnp.float32)
    for half in range(2):
        for now in range(2):
            work[now, half, :SUB, :] = margin
            work[now, half, SUB + full :, :] = margin

    def inside(r):
        return top <= r < top + rows

    def field(arr, z, r, half):
        if inside(r):
            blocks = ((dens, dens_side), (cot, cot_side))[arr]
            return blocks[half][z, r - top : r - top + SUB, :]
        d = reach[arr, z]
        before = r < top
        k = (top - r) // SUB - 1 if before else (r - top - rows) // SUB
        if half == 0:
            at = plan.row_at[arr, z]
            at = at + d - SUB * (k + 1) if before else at + SUB * k
            x, y = mine[at : at + SUB, :], other[at : at + SUB, :]
            return jnp.where(odd, x, y) if before else jnp.where(odd, y, x)
        found = []
        for part in range(2):
            w = plan.corner_width(d, k, part)
            if w > 0:
                place, cor = plan.corner_at[arr, z, k, part]
                x, y = cmine[place // 2], cother[place // 2]
                x = jnp.where(odd, x, y) if before else jnp.where(odd, y, x)
                found.append(turn(shift(x, -(cor + w)), place % 2, part != before))
        if len(found) < 2:
            return found[0] if found else jnp.ones((SUB, n), jnp.float32)
        return jnp.where(low != before, found[0], found[1])

    def tiles(depth):
        return range(top - up8(depth), top + rows + up8(depth), SUB)

    for z in range(nz):
        edge = up8(z)
        for r in tiles(2 * (nz - 1) - z):
            if top + edge <= r < top + rows - edge:
                continue
            total = (None, None) if z == 0 else cross(power, z - 1, r, lane)
            for half in range(2):
                layer(plan, z, r, half, field(0, z, r, half), total[half], *out)

    copies = [pltpu.make_async_copy(printed, printed_out, sems.at[nz])]
    copies[0].start()

    for z in range(nz - 1, -1, -1):
        for r in tiles(z):
            if z == nz - 1:
                spreads = (None, None)
            else:
                spreads = cross(work, (z + 1) % 2, r, lane)
            for half in range(2 if z > 0 else 1):
                adjoint = field(1, z, r, half) if z > 0 else cot[0, r - top : r - top + SUB, :]
                if spreads[half] is not None:
                    adjoint = adjoint + slope[z, half, r : r + SUB, :] * spreads[half]
                if z > 0:
                    work[z % 2, half, SUB + r : SUB + r + SUB, :] = adjoint * weight[z, half, r : r + SUB, :]
                if half == 0 and inside(r):
                    k = r - top
                    gradient[z, k : k + SUB, :] = adjoint * da[z, k : k + SUB, :]
        copies.append(pltpu.make_async_copy(gradient.at[z], gradient_out.at[z], sems.at[z]))
        copies[-1].start()
    for copy in copies:
        copy.wait()


def swap(axis, ours, theirs):
    count = lax.axis_size(axis)
    assert count % 2 == 0
    results = []
    for turn, x in enumerate((ours, theirs)):
        ends = [((i + turn) % count, (i + turn + 1) % count) for i in range(0, count, 2)]
        results.append(lax.ppermute(x, axis, [p for a, b in ends for p in ((a, b), (b, a))]))
    return results


def near(x):
    return pltpu.with_memory_space_constraint(x, pltpu.VMEM)


def call(body, outs, *args, flops=100000, limit=4):
    return pl.pallas_call(
        body,
        out_shape=[pltpu.VMEM(s, jnp.float32) for s in outs],
        in_specs=[VMEM] * len(args),
        out_specs=[VMEM] * len(outs),
        cost_estimate=pl.CostEstimate(flops=flops, bytes_accessed=flops, transcendentals=0),
        compiler_params=pltpu.CompilerParams(vmem_limit_bytes=limit << 20),
    )(*[near(x) for x in args])


def shards(density, cotangent):
    nz, rows, cols = density.shape
    plan = Plan(nz, rows, cols)
    part = functools.partial
    block = (nz, rows, cols)
    packed = (plan.row_len, cols)
    density, cotangent, ours, theirs = pl.pallas_call(
        part(fetch, plan),
        out_shape=[pltpu.VMEM(s, jnp.float32) for s in (block, block, packed, packed)],
        in_specs=[pl.BlockSpec(memory_space=pltpu.HBM)] * 2,
        out_specs=[VMEM] * 4,
        scratch_shapes=[pltpu.SemaphoreType.DMA((2,))],
        cost_estimate=pl.CostEstimate(flops=100000, bytes_accessed=1000000, transcendentals=0),
        compiler_params=pltpu.CompilerParams(vmem_limit_bytes=4 << 20),
    )(*[pltpu.with_memory_space_constraint(x, pltpu.HBM) for x in (density, cotangent)])
    near_rows = swap("gx", ours, theirs)
    ours, theirs = call(part(pack_columns, plan), [(plan.col_tiles, SUB, cols)] * 2, density, cotangent)
    sides = swap("gy", ours, theirs)
    ours, theirs = call(part(pack_corners, plan), [(plan.corner_tiles, SUB, cols)] * 2, *sides)
    corners = swap("gx", ours, theirs)
    full = rows + 2 * plan.halo
    power = (nz - 1, 2, full + 2 * SUB, cols)
    coef = (nz, 2, full, cols)
    kept = [power, coef, coef, block, block]
    dens_side, cot_side, *state = call(part(inner_body, plan), [block] * 2 + kept, density, *sides, limit=8)
    args = (density, cotangent, dens_side, cot_side, *near_rows, *corners, *state)
    *_, gradient, printed = pl.pallas_call(
        part(outer_body, plan),
        out_shape=[pltpu.VMEM(s, jnp.float32) for s in kept] + [jax.ShapeDtypeStruct(block, jnp.float32)] * 2,
        in_specs=[VMEM] * len(args),
        out_specs=[VMEM] * len(kept) + [pl.BlockSpec(memory_space=pltpu.HBM)] * 2,
        scratch_shapes=[
            pltpu.VMEM(block, jnp.float32),
            pltpu.VMEM((2, 2, full + 2 * SUB, cols), jnp.float32),
            pltpu.SemaphoreType.DMA((nz + 1,)),
        ],
        input_output_aliases={len(args) - len(kept) + i: i for i in range(len(kept))},
        cost_estimate=pl.CostEstimate(flops=10000000, bytes_accessed=1000000, transcendentals=0),
        compiler_params=pltpu.CompilerParams(vmem_limit_bytes=8 << 20),
    )(*[near(x) for x in args])
    return printed, gradient


def solution(mesh):
    placed = P(None, "gx", "gy")
    return jax.shard_map(
        shards,
        mesh=mesh,
        in_specs=(placed, placed),
        out_specs=(placed, placed),
        check_vma=False,
    )
```

```python
import functools
import math

import jax
import jax.numpy as jnp
from jax import lax
from jax.experimental import pallas as pl
from jax.experimental.pallas import tpu as pltpu
from jax.sharding import PartitionSpec as P


power_p = 20.0
root_q = 20.0 + math.log(5.0) / math.log(0.1)
smooth_eps = 0.0001
SUB = 8

VMEM = pl.BlockSpec(memory_space=pltpu.VMEM)


def up8(n):
    return -(-n // SUB) * SUB


class Plan:
    def __init__(self, layers, rows, cols):
        self.nz, self.rows, self.cols = layers, rows, cols
        self.fields = [(0, z, 2 * (layers - 1) - z) for z in range(layers)]
        self.fields += [(1, z, z) for z in range(layers - 1, 0, -1)]
        far = 2 * (layers - 1)
        self.halo = up8(far)
        line = sorted(self.fields, key=lambda f: f[2] % SUB != 0)
        even = sum(d % SUB == 0 for _, _, d in line)
        line = line[1:] + line[:1]
        line = line[even - 2 : even - 1] + line[: even - 2] + line[even - 1 :] if even >= 2 else line
        self.margin = 0 if even >= 2 else SUB
        self.row_at = {}
        at = self.margin
        for arr, z, d in line:
            self.row_at[arr, z] = at
            at += d
        self.row_end = at
        self.row_len = up8(at) + self.margin
        items = [((arr, z, r), d) for arr, z, d in self.fields for r in range(0, rows, SUB)]
        self.col_at, self.col_tiles = self.fit(items, both=True)
        items = []
        for arr, z, d in self.fields:
            for k in range(-(-(d - 1) // SUB)):
                for half in range(2):
                    if (w := self.corner_width(d, k, half)) > 0:
                        items.append(((arr, z, k, half), 2 * w))
        self.corner_at, bins = self.fit(items)
        self.corner_tiles = -(-bins // 2)

    def corner_width(self, d, k, half):
        return d - 1 - SUB * k - SUB // 2 * half

    def fit(self, items, both=False):
        room, widest, where = [], [], {}
        for key, width in sorted(items, key=lambda item: -item[1]):
            for tile, used in enumerate(room):
                if used + (widest[tile] if both else width) <= self.cols:
                    break
            else:
                tile = len(room)
                room.append(0)
                widest.append(width)
            where[key] = (tile, room[tile])
            room[tile] += width
        return where, len(room)


def shift(x, amount):
    amount %= x.shape[1]
    return x if amount == 0 else pltpu.roll(x, amount, 1)


def lanes_of(shape):
    return lax.broadcasted_iota(jnp.int32, shape, 1)


def odd_on(axis):
    return lax.rem(lax.axis_index(axis), 2) == 1


def fetch(plan, dens_in, cot_in, dens, cot, ours, theirs, sems):
    copies = [
        pltpu.make_async_copy(src, dst, sems.at[i])
        for i, (src, dst) in enumerate(((dens_in, dens), (cot_in, cot)))
    ]
    for copy in copies:
        copy.start()
    odd = odd_on("gx")
    for ref in (ours, theirs):
        if plan.margin > 0:
            ref[: plan.margin, :] = jnp.zeros((plan.margin, plan.cols), jnp.float32)
        if plan.row_len > plan.row_end:
            ref[plan.row_end :, :] = jnp.zeros((plan.row_len - plan.row_end, plan.cols), jnp.float32)
    for turn, copy in enumerate(copies):
        copy.wait()
        for arr, z, d in plan.fields:
            if arr == turn:
                src, at = (dens, cot)[arr], plan.row_at[arr, z]
                one, two = src[z, :d, :], src[z, plan.rows - d :, :]
                ours[at : at + d, :] = jnp.where(odd, one, two)
                theirs[at : at + d, :] = jnp.where(odd, two, one)


def pack_columns(plan, dens, cot, ours, theirs):
    n = plan.cols
    odd = odd_on("gy")
    lane = lanes_of((SUB, n))
    reach = {(arr, z): d for arr, z, d in plan.fields}
    for tile in range(plan.col_tiles):
        inside = [(at, key) for key, (t, at) in plan.col_at.items() if t == tile]
        one, two = None, None
        for at, (arr, z, r) in sorted(inside):
            d = reach[arr, z]
            x = shift((dens, cot)[arr][z, r : r + SUB, :], at)
            one = x if one is None else jnp.where(lane >= at, x, one)
            two = x if two is None else jnp.where((lane >= at - d) & (lane < at), x, two)
        ours[tile] = jnp.where(odd, one, two)
        theirs[tile] = jnp.where(odd, two, one)


def merge(odd, mine, other, at):
    n = mine.shape[1]
    lane = lanes_of(mine.shape)
    after = (lane >= at) & (lane < at + n // 2) if at <= n // 2 else (lane >= at) | (lane < at - n // 2)
    return jnp.where(after != odd, mine, other)


def pack_corners(plan, mine, other, ours, theirs):
    lane = lanes_of((SUB, plan.cols))
    odd_x, odd_y = odd_on("gx"), odd_on("gy")
    bins = 2 * plan.corner_tiles
    out = [[jnp.zeros(lane.shape, jnp.float32)] * bins, [jnp.zeros(lane.shape, jnp.float32)] * bins]
    reach = {(arr, z): d for arr, z, d in plan.fields}
    for (arr, z, k, half), (place, at) in sorted(plan.corner_at.items(), key=lambda item: item[1][1]):
        w = plan.corner_width(reach[arr, z], k, half)
        for way in range(2):
            r = SUB * k if way == 0 else plan.rows - SUB * (k + 1)
            ctile, cat = plan.col_at[arr, z, r]
            x = merge(odd_y, mine[ctile], other[ctile], cat)
            x = turn(shift(x, at + w - cat), half != way, place % 2)
            out[way][place] = x if at == 0 else jnp.where(lane >= at, x, out[way][place])
    low = lax.broadcasted_iota(jnp.int32, lane.shape, 0) < SUB // 2
    for tile in range(plan.corner_tiles):
        one, two = [jnp.where(low, out[way][2 * tile], out[way][2 * tile + 1]) for way in range(2)]
        ours[tile] = jnp.where(odd_x, one, two)
        theirs[tile] = jnp.where(odd_x, two, one)


def turn(x, src, dst):
    return x if bool(src) == bool(dst) else pltpu.roll(x, SUB // 2, 0)


def cross(ref, z, r, lane):
    n = lane.shape[1]
    b = SUB + r
    m, s = ref[z, 0, b : b + SUB, :], ref[z, 1, b : b + SUB, :]
    m1, s1 = pltpu.roll(m, 1, 1), pltpu.roll(s, 1, 1)
    m2, s2 = pltpu.roll(m, n - 1, 1), pltpu.roll(s, n - 1, 1)
    vm = m + ref[z, 0, b - 1 : b + SUB - 1, :] + ref[z, 0, b + 1 : b + SUB + 1, :]
    vs = s + ref[z, 1, b - 1 : b + SUB - 1, :] + ref[z, 1, b + 1 : b + SUB + 1, :]
    start, end = lane == 0, lane == n - 1
    hm = jnp.where(start, s1, m1) + jnp.where(end, s2, m2)
    hs = jnp.where(start, m1, s1) + jnp.where(end, m2, s2)
    return vm + hm, vs + hs


def layer(plan, z, r, half, density, total, power, slope, weight, da, printed):
    top, rows, coef = plan.halo, plan.rows, up8(z)
    if total is None:
        level = jnp.ones_like(density)
    else:
        lg = lax.log2(total)
        level = jnp.exp2(lg * jnp.float32(1.0 / root_q))
    diff = density - level
    square = diff * diff + smooth_eps
    inv = lax.rsqrt(square)
    value = 0.5 * (density + level - square * inv + math.sqrt(smooth_eps))
    p2 = value * value
    p4 = p2 * p2
    p16 = (p4 * p4) * (p4 * p4)
    if z < plan.nz - 1:
        power[z, half, SUB + r : SUB + r + SUB, :] = p16 * p4
    if top - coef <= r < top + rows + coef:
        u = diff * inv
        if z > 0 or half == 0:
            slope[z, half, r : r + SUB, :] = jnp.float32(0.5 * power_p / root_q) * (p16 * (p2 * value))
        if z > 0:
            ratio = jnp.exp2(lg * jnp.float32(1.0 / root_q - 1.0))
            weight[z, half, r : r + SUB, :] = (1.0 + u) * ratio
        if half == 0 and top <= r < top + rows:
            printed[z, r - top : r - top + SUB, :] = value
            da[z, r - top : r - top + SUB, :] = 0.5 - 0.5 * u


def inner_body(plan, dens, mine, other, dens_side, cot_side, power, slope, weight, da, printed):
    nz, rows, n, top = plan.nz, plan.rows, plan.cols, plan.halo
    lane = lanes_of((SUB, n))
    sides = (dens_side, cot_side)
    odd = odd_on("gy")
    for arr, z, d in plan.fields:
        for r in range(0, rows, SUB):
            tile, at = plan.col_at[arr, z, r]
            x = merge(odd, mine[tile], other[tile], at)
            sides[arr][z, r : r + SUB, :] = shift(x, -at)
    margin = jnp.ones((SUB, n), jnp.float32)
    out = (power, slope, weight, da, printed)
    for z in range(nz):
        if z < nz - 1:
            for half in range(2):
                for r in (0, top, SUB + top + rows, SUB + 2 * top + rows):
                    power[z, half, r : r + SUB, :] = margin
        skip = z // SUB * SUB
        for k in range(skip, rows - skip, SUB):
            total = (None, None) if z == 0 else cross(power, z - 1, top + k, lane)
            for half in range(2):
                density = (dens, dens_side)[half][z, k : k + SUB, :]
                layer(plan, z, top + k, half, density, total[half], *out)


def outer_body(
    plan, dens, cot, dens_side, cot_side, mine, other, cmine, cother, power_in, slope_in, weight_in, da_in, printed_in,
    power, slope, weight, da, printed, gradient_out, printed_out, gradient, work, sems,
):
    nz, rows, n, top = plan.nz, plan.rows, plan.cols, plan.halo
    lane = lanes_of((SUB, n))
    low = lax.broadcasted_iota(jnp.int32, lane.shape, 0) < SUB // 2
    full = top + rows + top
    reach = {(arr, z): d for arr, z, d in plan.fields}
    odd = odd_on("gx")
    out = (power, slope, weight, da, printed)

    margin = jnp.ones((SUB, n), jnp.float32)
    for half in range(2):
        for now in range(2):
            work[now, half, :SUB, :] = margin
            work[now, half, SUB + full :, :] = margin

    def inside(r):
        return top <= r < top + rows

    def field(arr, z, r, half):
        if inside(r):
            blocks = ((dens, dens_side), (cot, cot_side))[arr]
            return blocks[half][z, r - top : r - top + SUB, :]
        d = reach[arr, z]
        before = r < top
        k = (top - r) // SUB - 1 if before else (r - top - rows) // SUB
        if half == 0:
            at = plan.row_at[arr, z]
            at = at + d - SUB * (k + 1) if before else at + SUB * k
            x, y = mine[at : at + SUB, :], other[at : at + SUB, :]
            return jnp.where(odd, x, y) if before else jnp.where(odd, y, x)
        found = []
        for part in range(2):
            w = plan.corner_width(d, k, part)
            if w > 0:
                place, cor = plan.corner_at[arr, z, k, part]
                x, y = cmine[place // 2], cother[place // 2]
                x = jnp.where(odd, x, y) if before else jnp.where(odd, y, x)
                found.append(turn(shift(x, -(cor + w)), place % 2, part != before))
        if len(found) < 2:
            return found[0] if found else jnp.ones((SUB, n), jnp.float32)
        return jnp.where(low != before, found[0], found[1])

    def tiles(depth):
        return range(top - up8(depth), top + rows + up8(depth), SUB)

    for z in range(nz):
        edge = up8(z)
        left = [r for r in tiles(2 * (nz - 1) - z) if not top + edge <= r < top + rows - edge]
        m = len(left) // 2
        for r in [r for pair in zip(left[:m], left[m:]) for r in pair] + left[2 * m :]:
            total = (None, None) if z == 0 else cross(power, z - 1, r, lane)
            for half in range(2):
                layer(plan, z, r, half, field(0, z, r, half), total[half], *out)

    copies = [pltpu.make_async_copy(printed, printed_out, sems.at[nz])]
    copies[0].start()

    for z in range(nz - 1, -1, -1):
        for r in tiles(z):
            if z == nz - 1:
                spreads = (None, None)
            else:
                spreads = cross(work, (z + 1) % 2, r, lane)
            for half in range(2 if z > 0 else 1):
                adjoint = field(1, z, r, half) if z > 0 else cot[0, r - top : r - top + SUB, :]
                if spreads[half] is not None:
                    adjoint = adjoint + slope[z, half, r : r + SUB, :] * spreads[half]
                if z > 0:
                    work[z % 2, half, SUB + r : SUB + r + SUB, :] = adjoint * weight[z, half, r : r + SUB, :]
                if half == 0 and inside(r):
                    k = r - top
                    gradient[z, k : k + SUB, :] = adjoint * da[z, k : k + SUB, :]
        copies.append(pltpu.make_async_copy(gradient.at[z], gradient_out.at[z], sems.at[z]))
        copies[-1].start()
    for copy in copies:
        copy.wait()


def swap(axis, ours, theirs):
    count = lax.axis_size(axis)
    assert count % 2 == 0
    results = []
    for turn, x in enumerate((ours, theirs)):
        ends = [((i + turn) % count, (i + turn + 1) % count) for i in range(0, count, 2)]
        results.append(lax.ppermute(x, axis, [p for a, b in ends for p in ((a, b), (b, a))]))
    return results


def near(x):
    return pltpu.with_memory_space_constraint(x, pltpu.VMEM)


def call(body, outs, *args, flops=100000, limit=4):
    return pl.pallas_call(
        body,
        out_shape=[pltpu.VMEM(s, jnp.float32) for s in outs],
        in_specs=[VMEM] * len(args),
        out_specs=[VMEM] * len(outs),
        cost_estimate=pl.CostEstimate(flops=flops, bytes_accessed=flops, transcendentals=0),
        compiler_params=pltpu.CompilerParams(vmem_limit_bytes=limit << 20),
    )(*[near(x) for x in args])


def shards(density, cotangent):
    nz, rows, cols = density.shape
    plan = Plan(nz, rows, cols)
    part = functools.partial
    block = (nz, rows, cols)
    packed = (plan.row_len, cols)
    density, cotangent, ours, theirs = pl.pallas_call(
        part(fetch, plan),
        out_shape=[pltpu.VMEM(s, jnp.float32) for s in (block, block, packed, packed)],
        in_specs=[pl.BlockSpec(memory_space=pltpu.HBM)] * 2,
        out_specs=[VMEM] * 4,
        scratch_shapes=[pltpu.SemaphoreType.DMA((2,))],
        cost_estimate=pl.CostEstimate(flops=100000, bytes_accessed=1000000, transcendentals=0),
        compiler_params=pltpu.CompilerParams(vmem_limit_bytes=4 << 20),
    )(*[pltpu.with_memory_space_constraint(x, pltpu.HBM) for x in (density, cotangent)])
    near_rows = swap("gx", ours, theirs)
    ours, theirs = call(part(pack_columns, plan), [(plan.col_tiles, SUB, cols)] * 2, density, cotangent)
    sides = swap("gy", ours, theirs)
    ours, theirs = call(part(pack_corners, plan), [(plan.corner_tiles, SUB, cols)] * 2, *sides)
    corners = swap("gx", ours, theirs)
    full = rows + 2 * plan.halo
    power = (nz - 1, 2, full + 2 * SUB, cols)
    coef = (nz, 2, full, cols)
    kept = [power, coef, coef, block, block]
    dens_side, cot_side, *state = call(part(inner_body, plan), [block] * 2 + kept, density, *sides, limit=8)
    args = (density, cotangent, dens_side, cot_side, *near_rows, *corners, *state)
    *_, gradient, printed = pl.pallas_call(
        part(outer_body, plan),
        out_shape=[pltpu.VMEM(s, jnp.float32) for s in kept] + [jax.ShapeDtypeStruct(block, jnp.float32)] * 2,
        in_specs=[VMEM] * len(args),
        out_specs=[VMEM] * len(kept) + [pl.BlockSpec(memory_space=pltpu.HBM)] * 2,
        scratch_shapes=[
            pltpu.VMEM(block, jnp.float32),
            pltpu.VMEM((2, 2, full + 2 * SUB, cols), jnp.float32),
            pltpu.SemaphoreType.DMA((nz + 1,)),
        ],
        input_output_aliases={len(args) - len(kept) + i: i for i in range(len(kept))},
        cost_estimate=pl.CostEstimate(flops=10000000, bytes_accessed=1000000, transcendentals=0),
        compiler_params=pltpu.CompilerParams(vmem_limit_bytes=8 << 20),
    )(*[near(x) for x in args])
    return printed, gradient


def solution(mesh):
    placed = P(None, "gx", "gy")
    return jax.shard_map(
        shards,
        mesh=mesh,
        in_specs=(placed, placed),
        out_specs=(placed, placed),
        check_vma=False,
    )
```
